128 devices in a mesh: rows: 128 (over x, z, y, core).
Axes of the slice: x: 4, y: 4, z: 4, core: 2. Of those that a mesh axis runs over, the one named last changes fastest.
Arguments:
- tile_values: float32 [26624, 128, 128], P('rows'), as said below
- tile_row: int32 [26624], P('rows'), may hold values from 0 to 15, as said below
- tile_slot: int32 [26624], P('rows'), may hold values from 0 to 143, as said below
- tile_count: int32 [128], P('rows'), may hold values from 144 to 208, as said below
- requests: int32 [128, 128, 1], P('rows'), may hold values from 0 to 15
- right_side: float32 [2048, 4, 128], P('rows')
Outputs:
- solution: float32 [2048, 4, 128], P('rows')
- hessenberg: float32 [4, 4, 3], replicated
The draws below stay inside these ranges and needn't reach their ends.
Inputs may be any that keep to these rules, and one draw needn't show every extreme that they name: `tile_row`: tile t < 16 of every device lies in block row t; it is the diagonal tile of that row. `tile_slot`: slot s < 16 is the device's own block s; slot 16 + o + q is the q-th block requested from device o; tile t < 144 of every device uses slot t. `tile_count`: some device uses all 208 slots. requests[d, o, q] is a block index among device o's 16 block rows. `tile_values`: tile t < 16 of every device holds the diagonal block of its row.
All inputs are finite; a program needn't handle non-finite values.
Results may differ from the reference program's by a relative error of at most 0.0003.
Values sent between devices are 32-bit elements; how exact they have to be, the bound alone decides.
No kernel may reach another device: no remote copies, remote signals or barrier semaphores. Data moves between devices by JAX's collectives and lax.ppermute only.
A program may use at most 64 MiB of HBM per device.

```python
import jax
import jax.numpy as jnp
from jax import lax

BS = 128
RB = 16
NRHS = 4
REQ = 1
EXTRA = 64
ITERS = 3
BLOCKS = 2048
SLOTS = 144
TILES_DEV = 208
NTILES = 26624
N_ROWS = 128


def draw_tile_values(key, part):
    position = jnp.arange(NTILES, dtype=jnp.int32)
    diagonal_tile = position % TILES_DEV < RB
    spread = 0.7 / jnp.sqrt(jnp.float32(BS * TILES_DEV / RB))
    noise_key = jax.random.fold_in(key, 11)
    scale_key = jax.random.fold_in(key, 12)
    noise = jax.random.normal(noise_key, (NTILES, BS, BS), jnp.float32)
    scales = jax.random.uniform(scale_key, (NTILES, BS), jnp.float32, 1.0, 2.0)
    boosted = jnp.where(diagonal_tile[:, None], scales, 0.0)
    identity = jnp.eye(BS, dtype=jnp.float32)
    return noise * spread + boosted[:, :, None] * identity[None, :, :]


def draw_tile_row(key, part):
    position = jnp.arange(NTILES, dtype=jnp.int32) % TILES_DEV
    chosen = jax.random.randint(jax.random.fold_in(key, 21), (NTILES,), 0, RB, dtype=jnp.int32)
    return jnp.where(position < RB, position, chosen).astype(jnp.int32)


def draw_tile_slot(key, part):
    position = jnp.arange(NTILES, dtype=jnp.int32) % TILES_DEV
    chosen = jax.random.randint(jax.random.fold_in(key, 31), (NTILES,), 0, SLOTS, dtype=jnp.int32)
    return jnp.where(position < SLOTS, position, chosen).astype(jnp.int32)


def draw_tile_count(key, part):
    devices = NTILES // TILES_DEV
    level = jax.random.randint(jax.random.fold_in(key, 41), (devices,), 0, 65, dtype=jnp.int32)
    counts = SLOTS + EXTRA * level * level // 4096
    busiest = jax.random.randint(jax.random.fold_in(key, 42), (), 0, devices, dtype=jnp.int32)
    return jnp.where(jnp.arange(devices, dtype=jnp.int32) == busiest, TILES_DEV, counts).astype(jnp.int32)


def draw_right_side(key, part):
    devices = BLOCKS // RB
    owner_of = (jnp.arange(BLOCKS, dtype=jnp.int32) // RB).astype(jnp.float32)
    ramp = 1.0 + 2.0 * owner_of / max(devices - 1, 1)
    rough = jnp.exp(jax.random.uniform(jax.random.fold_in(key, 51), (BLOCKS, NRHS, 1), jnp.float32, -0.7, 0.7))
    values = jax.random.normal(jax.random.fold_in(key, 52), (BLOCKS, NRHS, BS), jnp.float32)
    return values * rough * ramp[:, None, None]


def set_ends(result, stream_key, low, high):
    place = [jax.random.randint(jax.random.fold_in(stream_key, axis), (), 0, length) for axis, length in enumerate(result.shape)]
    longest = result.shape.index(max(result.shape))
    neighbour = place[:longest] + [(place[longest] + 1) % result.shape[longest]] + place[longest + 1:]
    return result.at[tuple(place)].set(low).at[tuple(neighbour)].set(high)


def setup_inputs(seed: int = 0) -> dict:
    key_of = jax.random.split(jax.random.key(seed), 7)
    return {
        "tile_values": draw_tile_values(jax.random.fold_in(key_of[6], 71), 0),
        "tile_row": draw_tile_row(jax.random.fold_in(key_of[6], 71), 0),
        "tile_slot": draw_tile_slot(jax.random.fold_in(key_of[6], 71), 0),
        "tile_count": draw_tile_count(jax.random.fold_in(key_of[6], 71), 0),
        "requests": set_ends(jax.random.randint(key_of[4], (N_ROWS, N_ROWS, REQ), 0, RB), jax.random.fold_in(key_of[4], 1), 0, RB - 1).astype(jnp.int32),
        "right_side": draw_right_side(jax.random.fold_in(key_of[6], 71), 0),
    }


epsilon = 1e-06
highest = lax.Precision.HIGHEST

def least_squares(hessenberg, beta_norm):
    krylov = hessenberg.shape[2]
    triangle = hessenberg
    target = jnp.zeros((hessenberg.shape[0], krylov + 1), jnp.float32).at[:, 0].set(beta_norm)
    cosines = []
    sine_list = []
    for column in range(krylov):
        column_vals = triangle[:, :, column]
        for earlier in range(column):
            first_entry = column_vals[:, earlier]
            second = column_vals[:, earlier + 1]
            column_vals = column_vals.at[:, earlier].set(cosines[earlier] * first_entry + sine_list[earlier] * second)
            column_vals = column_vals.at[:, earlier + 1].set(cosines[earlier] * second - sine_list[earlier] * first_entry)
        first_entry = column_vals[:, column]
        second = column_vals[:, column + 1]
        radius = jnp.sqrt(first_entry * first_entry + second * second)
        cosine = first_entry / radius
        sine_term = second / radius
        cosines.append(cosine)
        sine_list.append(sine_term)
        column_vals = column_vals.at[:, column].set(radius).at[:, column + 1].set(0.0)
        triangle = triangle.at[:, :, column].set(column_vals)
        leading = target[:, column]
        target = target.at[:, column].set(cosine * leading).at[:, column + 1].set(-sine_term * leading)
    weights = jnp.zeros((hessenberg.shape[0], krylov), jnp.float32)
    for column in reversed(range(krylov)):
        partial_sum = target[:, column] - lax.optimization_barrier(jnp.sum(triangle[:, column, column + 1:krylov] * weights[:, column + 1:], axis=1))
        weights = weights.at[:, column].set(partial_sum / triangle[:, column, column])
    return weights

def reference(tile_values, tile_row, tile_slot, tile_count, requests, right_side):
    tile_total = tile_slot.shape[0]
    position = jnp.arange(tile_total, dtype=jnp.int32)
    device = (position // TILES_DEV).astype(jnp.int32)
    shifted = jnp.maximum(tile_slot - RB, 0)
    owner_index = (shifted // REQ).astype(jnp.int32)
    within = (shifted % REQ).astype(jnp.int32)
    remote = requests[device, owner_index, within]
    columns = jnp.where(tile_slot < RB, device * RB + tile_slot, owner_index * RB + remote).astype(jnp.int32)
    rows_global = (device * RB + tile_row).astype(jnp.int32)
    live_mask = (position % TILES_DEV < tile_count[device]).astype(jnp.float32)

    def apply_matrix(vector):
        picked = vector[columns]
        products = jnp.einsum('tij,tkj->tki', tile_values, picked, precision=highest)
        products = products * live_mask[:, None, None]
        return jax.ops.segment_sum(products, rows_global, num_segments=vector.shape[0])
    beta_norm = jnp.sqrt(lax.optimization_barrier(jnp.sum(right_side * right_side, axis=(0, 2))) + epsilon)
    basis_list = [right_side / beta_norm[None, :, None]]
    hessenberg = jnp.zeros((right_side.shape[1], ITERS + 1, ITERS), jnp.float32)
    for column in range(ITERS):
        candidate = apply_matrix(basis_list[column])
        for earlier in range(column + 1):
            projection = lax.optimization_barrier(jnp.sum(candidate * basis_list[earlier], axis=(0, 2)))
            hessenberg = hessenberg.at[:, earlier, column].set(projection)
            candidate = candidate - projection[None, :, None] * basis_list[earlier]
        length = jnp.sqrt(lax.optimization_barrier(jnp.sum(candidate * candidate, axis=(0, 2))) + epsilon)
        hessenberg = hessenberg.at[:, column + 1, column].set(length)
        if column + 1 < ITERS:
            basis_list.append(candidate / length[None, :, None])
    weights = least_squares(hessenberg, beta_norm)
    stacked = jnp.stack(basis_list)
    solution = jnp.einsum('kj,jrki->rki', weights, stacked, precision=highest)
    return (solution, hessenberg)
```

```python
import functools

import jax
import jax.numpy as jnp
from jax import lax
from jax.experimental import pallas as pl
from jax.experimental.pallas import tpu as pltpu
from jax.sharding import Mesh
from jax.sharding import PartitionSpec as P

ITERS = 3
NRHS = 4
ROWS = ("rows_0", "rows_1", "rows_2", "rows_3")
EPSILON = 1e-06

CHUNK = 16
BUFFERS = 4
UNROLL = 26
PART = 13
TOTALS = 8
MIB = 1 << 20

WW = 3
GRAM = 4

VMEM = pl.BlockSpec(memory_space=pltpu.VMEM)
SMEM = pl.BlockSpec(memory_space=pltpu.SMEM)
HBM = pl.BlockSpec(memory_space=pltpu.HBM)


def split2(x):
    high = x.astype(jnp.bfloat16)
    return high, (x - high.astype(jnp.float32)).astype(jnp.bfloat16)


def prepare_kernel(count, tiles, weights, done, buffer, arrived, packed, left):
    chunks = tiles.shape[0] // CHUNK
    pairs = CHUNK // 2

    def fetch(chunk):
        slot = lax.rem(chunk, BUFFERS)
        return pltpu.make_async_copy(
            tiles.at[pl.ds(chunk * CHUNK, CHUNK)], buffer.at[slot], arrived.at[slot]
        )

    def put(chunk):
        slot = lax.rem(chunk, 2)
        return pltpu.make_async_copy(
            packed.at[slot], weights.at[pl.ds(chunk * pairs, pairs)], left.at[slot]
        )

    for chunk in range(BUFFERS - 1):
        fetch(chunk).start()
    done[...] = jnp.zeros_like(done)
    live = count[0]

    def body(chunk, carry):
        @pl.when(chunk + BUFFERS - 1 < chunks)
        def _():
            fetch(chunk + BUFFERS - 1).start()

        @pl.when(chunk >= 2)
        def _():
            put(chunk - 2).wait()

        fetch(chunk).wait()
        slot = lax.rem(chunk, BUFFERS)
        target = lax.rem(chunk, 2)
        for local in range(CHUNK):
            tile = buffer[slot, local]
            tile = jnp.where(chunk * CHUNK + local < live, tile, 0.0)
            high, low = split2(tile.T)
            lanes = pl.ds((local % 2) * 128, 128)
            packed[target, local // 2, pl.ds(0, 128), lanes] = high
            packed[target, local // 2, pl.ds(128, 128), lanes] = low
        put(chunk).start()
        return carry

    lax.fori_loop(0, chunks, body, 0)
    put(chunks - 2).wait()
    put(chunks - 1).wait()


def lane_sums(terms):
    lane = lax.broadcasted_iota(jnp.int32, (8, 128), 1)
    row = jnp.zeros((8, 128), jnp.float32)
    for place, term in terms.items():
        partial = jnp.sum(term[:8] + term[8:], axis=1, keepdims=True)
        row = row + jnp.where(lane == place, partial, 0.0)
    return jnp.sum(row, axis=0, keepdims=True)


def write_outgoing(outgoing, onehot, blocks, sums):
    wide = jnp.concatenate(blocks, axis=1)
    first = wide.astype(jnp.bfloat16)
    rest = wide - first.astype(jnp.float32)
    second, third = split2(rest)
    parts = jnp.concatenate([first, second, third], axis=0)
    hot = onehot[:, :16]
    chosen = jnp.dot(
        jnp.concatenate([hot, hot, hot], axis=1), parts, preferred_element_type=jnp.float32
    )
    devices = onehot.shape[0]
    stride = NRHS + 1
    for system in range(NRHS):
        outgoing[pl.ds(system, devices, stride=stride), :] = chosen[
            :, system * 128 : (system + 1) * 128
        ]
    outgoing[pl.ds(NRHS, devices, stride=stride), :] = jnp.broadcast_to(sums, (devices, 128))


def first_kernel(right_side, asked, prepared, onehot, outgoing):
    del prepared
    lane = lax.broadcasted_iota(jnp.int32, asked.shape, 1)
    hot = (asked[...] == lane).astype(jnp.float32).astype(jnp.bfloat16)
    onehot[...] = hot
    blocks = [right_side[pl.ds(k, 16, stride=NRHS), :] for k in range(NRHS)]
    sums = lane_sums({WW * NRHS + k: blocks[k] * blocks[k] for k in range(NRHS)})
    write_outgoing(outgoing, hot, blocks, sums)


def coefficients(rows, system):
    def entry(row, group):
        place = group * NRHS + system
        return jnp.broadcast_to(row[:, place : place + 1], (1, 128))

    beta = jnp.sqrt(entry(rows[0], WW) + EPSILON)
    columns = []
    gram = {}
    for column, row in enumerate(rows[1:]):
        dots = [entry(row, i) for i in range(column + 1)]
        for i in range(column + 1):
            gram[i, column] = gram[column, i] = entry(row, GRAM + i)
        h = []
        for i in range(column + 1):
            value = dots[i]
            for l in range(i):
                value = value - h[l] * gram[l, i]
            h.append(value)
        left = entry(row, WW)
        for i in range(column + 1):
            left = left - h[i] * dots[i]
        for i in range(column + 1):
            residue = dots[i]
            for l in range(column + 1):
                residue = residue - h[l] * gram[l, i]
            left = left - h[i] * residue
        columns.append((h, jnp.sqrt(jnp.maximum(left, 0.0) + EPSILON)))
    return beta, columns


def step_kernel(step, last, *refs):
    refs = list(refs)
    slots, rows_of, stored, onehot, incoming, own = refs[:6]
    del refs[:6]
    earlier_sums = refs[:step]
    del refs[:step]
    earlier = refs[:step]
    del refs[:step]
    basis, sums_out, product, outgoing = refs[:4]
    del refs[:4]
    parts = stored.shape[0] // PART
    weights = stored
    if step == 0:
        weights, arrived = refs.pop(0), refs.pop()

        def fetch(part):
            place = pl.ds(part * PART, PART)
            return pltpu.make_async_copy(stored.at[place], weights.at[place], arrived.at[part])

        for part in range(parts):
            fetch(part).start()
    table, *totals = refs
    devices = onehot.shape[0]
    blocks = 16
    all_blocks = blocks + devices
    stride = NRHS + 1

    sums = jnp.sum(incoming[pl.ds(NRHS, devices, stride=stride), :], axis=0, keepdims=True)
    sums_out[...] = jnp.broadcast_to(sums, (8, 128))
    sums_rows = [ref[pl.ds(0, 1), :] for ref in earlier_sums] + [sums]
    for total in totals:
        total[...] = jnp.zeros_like(total)
    for k in range(NRHS):
        beta, columns = coefficients(sums_rows, k)
        if step == 0:
            scale = 1.0 / beta
            mine = own[pl.ds(k, blocks, stride=NRHS), :]
            h = []
        else:
            h, length = columns[-1]
            scale = 1.0 / length
            mine = own[pl.ds(k * blocks, blocks), :]
        theirs = incoming[pl.ds(k, devices, stride=stride), :]
        for start, size, value in ((0, blocks, mine), (blocks, devices, theirs)):
            for i in range(step):
                value = value - h[i] * earlier[i][pl.ds(k * all_blocks + start, size), :]
            value = value * scale
            basis[pl.ds(k * all_blocks + start, size), :] = value
            high = value.astype(jnp.bfloat16).astype(jnp.float32)
            table[pl.ds(start * 8 + k, size, stride=8), :] = high
            table[pl.ds(start * 8 + NRHS + k, size, stride=8), :] = value - high

    pairs = weights.shape[0]

    def body(trip, carry):
        for local in range(UNROLL):
            pair = trip * UNROLL + local
            if step == 0 and local % PART == 0:
                fetch(trip * (UNROLL // PART) + local // PART).wait()
            picked = [
                table[pl.ds(pl.multiple_of(slots[2 * pair + side] * 8, 8), 8), :]
                for side in range(2)
            ]
            left = jnp.concatenate(picked, axis=0).astype(jnp.bfloat16)
            left = jnp.concatenate([left, left], axis=1)
            result = jnp.dot(left, weights[pair], preferred_element_type=jnp.float32)
            for side in range(2):
                total = totals[(2 * local + side) % TOTALS]
                place = pl.ds(pl.multiple_of(rows_of[2 * pair + side] * 8, 8), 8)
                total[place, :] += result[side * 8 : side * 8 + 8, side * 128 : side * 128 + 128]
        return carry

    lax.fori_loop(0, pairs // UNROLL, body, 0)

    total = totals[0]
    summed = total[...]
    for other in totals[1:]:
        summed = summed + other[...]
    total[...] = summed
    new = [
        total[pl.ds(k, blocks, stride=8), :] + total[pl.ds(NRHS + k, blocks, stride=8), :]
        for k in range(NRHS)
    ]
    terms = {}
    for k in range(NRHS):
        product[pl.ds(k * blocks, blocks), :] = new[k]
        latest = basis[pl.ds(k * all_blocks, blocks), :]
        known = [ref[pl.ds(k * all_blocks, blocks), :] for ref in earlier] + [latest]
        for i, vector in enumerate(known):
            terms[i * NRHS + k] = vector * new[k]
            terms[(GRAM + i) * NRHS + k] = vector * latest
        terms[WW * NRHS + k] = new[k] * new[k]
    local = lane_sums(terms)
    if last:
        outgoing[...] = jnp.broadcast_to(local, outgoing.shape)
    else:
        write_outgoing(outgoing, onehot[...], new, local)


def weights_of(beta, columns):
    rotations = []
    triangle = []
    target = [beta]
    for column, (h, length) in enumerate(columns):
        values = list(h) + [length]
        for earlier, (cosine, sine) in enumerate(rotations):
            first, second = values[earlier], values[earlier + 1]
            values[earlier] = cosine * first + sine * second
            values[earlier + 1] = cosine * second - sine * first
        first, second = values[column], values[column + 1]
        radius = jnp.sqrt(first * first + second * second)
        cosine, sine = first / radius, second / radius
        rotations.append((cosine, sine))
        triangle.append(values[:column] + [radius])
        leading = target[column]
        target[column] = cosine * leading
        target.append(-sine * leading)
    size = len(columns)
    weights = [None] * size
    for column in reversed(range(size)):
        value = target[column]
        for later in range(column + 1, size):
            value = value - triangle[later][column] * weights[later]
        weights[column] = value / triangle[column][column]
    return weights


def final_kernel(incoming, sums0, sums1, sums2, basis0, basis1, basis2, solution, hessenberg):
    blocks = 16
    all_blocks = basis0.shape[0] // NRHS
    sums = jnp.sum(incoming[...], axis=0, keepdims=True)
    rows = [ref[pl.ds(0, 1), :] for ref in (sums0, sums1, sums2)] + [sums]
    row_id = lax.broadcasted_iota(jnp.int32, (8, 128), 0)
    lane = lax.broadcasted_iota(jnp.int32, (8, 128), 1)
    tables = [jnp.zeros((8, 128), jnp.float32)] * ITERS
    for k in range(NRHS):
        beta, columns = coefficients(rows, k)
        weights = weights_of(beta, columns)
        value = jnp.zeros((blocks, 128), jnp.float32)
        for weight, basis in zip(weights, (basis0, basis1, basis2)):
            value = value + weight * basis[pl.ds(k * all_blocks, blocks), :]
        solution[pl.ds(k, blocks, stride=NRHS), :] = value
        for column, (h, length) in enumerate(columns):
            for i, entry in enumerate(list(h) + [length]):
                tables[column] = jnp.where((row_id == k) & (lane == i), entry, tables[column])
    for column in range(ITERS):
        hessenberg[column] = tables[column][:NRHS, : ITERS + 1]


def params(limit):
    return pltpu.CompilerParams(vmem_limit_bytes=limit * MIB)


def exchange(outgoing):
    size = outgoing.shape[0]
    moved = lax.all_to_all(
        outgoing.reshape(size, 1, 128), ROWS, split_axis=0, concat_axis=0, tiled=True
    )
    return moved.reshape(size, 128)


def on_device(tile_values, tile_row, tile_slot, tile_count, requests, right_side):
    devices = lax.axis_size(ROWS)
    tiles = tile_values.shape[0]
    blocks = right_side.shape[0]
    all_blocks = blocks + devices
    f32 = jnp.float32
    flat = right_side.reshape(blocks * NRHS, 128)
    asked = exchange(jnp.broadcast_to(requests[0], (devices, 128)))
    weights, prepared = pl.pallas_call(
        prepare_kernel,
        out_shape=(
            pltpu.HBM((tiles // 2, 256, 256), jnp.bfloat16),
            jax.ShapeDtypeStruct((8, 128), f32),
        ),
        in_specs=[SMEM, HBM],
        out_specs=(HBM, VMEM),
        scratch_shapes=[
            pltpu.VMEM((BUFFERS, CHUNK, 128, 128), f32),
            pltpu.SemaphoreType.DMA((BUFFERS,)),
            pltpu.VMEM((2, CHUNK // 2, 256, 256), jnp.bfloat16),
            pltpu.SemaphoreType.DMA((2,)),
        ],
        compiler_params=params(24),
        cost_estimate=pl.CostEstimate(
            flops=100_000_000, bytes_accessed=tiles * 65536, transcendentals=0
        ),
        name="prepare",
    )(tile_count, pltpu.with_memory_space_constraint(tile_values, pltpu.HBM))
    onehot, outgoing = pl.pallas_call(
        first_kernel,
        out_shape=(
            jax.ShapeDtypeStruct((devices, 128), jnp.bfloat16),
            jax.ShapeDtypeStruct((devices * (NRHS + 1), 128), f32),
        ),
        in_specs=[VMEM, VMEM, VMEM],
        out_specs=(VMEM, VMEM),
        compiler_params=params(8),
        name="first",
    )(flat, asked, prepared)
    sums, basis = [], []
    own = flat
    for step in range(ITERS):
        last = step == ITERS - 1
        incoming = exchange(outgoing)
        shapes = [
            jax.ShapeDtypeStruct((NRHS * all_blocks, 128), f32),
            jax.ShapeDtypeStruct((8, 128), f32),
            jax.ShapeDtypeStruct((NRHS * blocks, 128), f32),
            jax.ShapeDtypeStruct((devices if last else devices * (NRHS + 1), 128), f32),
        ]
        scratch = [pltpu.VMEM((all_blocks * 8, 128), f32)]
        scratch += [pltpu.VMEM((blocks * 8, 128), f32)] * TOTALS
        if step == 0:
            shapes.append(pltpu.VMEM(weights.shape, weights.dtype))
            scratch.append(pltpu.SemaphoreType.DMA((weights.shape[0] // PART,)))
            weights = pltpu.with_memory_space_constraint(weights, pltpu.HBM)
        vector, row, own, outgoing, *kept = pl.pallas_call(
            functools.partial(step_kernel, step, last),
            out_shape=shapes,
            in_specs=[SMEM, SMEM, HBM if step == 0 else VMEM] + [VMEM] * (3 + 2 * step),
            out_specs=[VMEM] * len(shapes),
            scratch_shapes=scratch,
            compiler_params=params(24),
            name=f"step{step}",
        )(tile_slot, tile_row, weights, onehot, incoming, own, *sums, *basis)
        if kept:
            weights = kept[0]
        sums.append(row)
        basis.append(vector)
    incoming = exchange(outgoing)
    solution, hessenberg = pl.pallas_call(
        final_kernel,
        out_shape=(
            jax.ShapeDtypeStruct((blocks * NRHS, 128), f32),
            jax.ShapeDtypeStruct((ITERS, NRHS, ITERS + 1), f32),
        ),
        in_specs=[VMEM] * (1 + 2 * ITERS),
        out_specs=(VMEM, VMEM),
        compiler_params=params(8),
        name="final",
    )(incoming, *sums, *basis)
    return solution.reshape(blocks, NRHS, 128), hessenberg.transpose(1, 2, 0)


def solution(mesh):
    finer = Mesh(mesh.devices.reshape(4, 4, 4, 2), ROWS)
    placed = (
        P(ROWS, None, None),
        P(ROWS),
        P(ROWS),
        P(ROWS),
        P(ROWS, None, None),
        P(ROWS, None, None),
    )
    return jax.shard_map(
        on_device,
        mesh=finer,
        in_specs=placed,
        out_specs=(P(ROWS, None, None), P()),
        check_vma=False,
    )
```

```python
import functools

import jax
import jax.numpy as jnp
from jax import lax
from jax.experimental import pallas as pl
from jax.experimental.pallas import tpu as pltpu
from jax.sharding import Mesh
from jax.sharding import PartitionSpec as P

ITERS = 3
NRHS = 4
ROWS = ("rows_0", "rows_1", "rows_2", "rows_3")
EPSILON = 1e-06

CHUNK = 16
BUFFERS = 4
UNROLL = 26
TOTALS = 8
MIB = 1 << 20

WW = 3
GRAM = 4

VMEM = pl.BlockSpec(memory_space=pltpu.VMEM)
SMEM = pl.BlockSpec(memory_space=pltpu.SMEM)
HBM = pl.BlockSpec(memory_space=pltpu.HBM)


def split2(x):
    high = x.astype(jnp.bfloat16)
    return high, (x - high.astype(jnp.float32)).astype(jnp.bfloat16)


def lane_sums(terms):
    lane = lax.broadcasted_iota(jnp.int32, (8, 128), 1)
    row = jnp.zeros((8, 128), jnp.float32)
    for place, term in terms.items():
        partial = jnp.sum(term[:8] + term[8:], axis=1, keepdims=True)
        row = row + jnp.where(lane == place, partial, 0.0)
    return jnp.sum(row, axis=0, keepdims=True)


def write_outgoing(outgoing, onehot, blocks, sums):
    wide = jnp.concatenate(blocks, axis=1)
    first = wide.astype(jnp.bfloat16)
    rest = wide - first.astype(jnp.float32)
    second, third = split2(rest)
    parts = jnp.concatenate([first, second, third], axis=0)
    hot = onehot[:, :16]
    chosen = jnp.dot(
        jnp.concatenate([hot, hot, hot], axis=1), parts, preferred_element_type=jnp.float32
    )
    devices = onehot.shape[0]
    stride = NRHS + 1
    for system in range(NRHS):
        outgoing[pl.ds(system, devices, stride=stride), :] = chosen[
            :, system * 128 : (system + 1) * 128
        ]
    outgoing[pl.ds(NRHS, devices, stride=stride), :] = jnp.broadcast_to(sums, (devices, 128))


def begin_kernel(*refs):
    count, *given = refs[:5]
    wanted, own, *kept = refs[5:10]
    requests, right_side, copied = refs[10:]
    held = (requests, right_side)
    kept[-1][0] = count[0]
    copies = [
        pltpu.make_async_copy(source, target, copied.at[place])
        for place, (source, target) in enumerate(zip(given, [*held, *kept[:2]]))
    ]
    for copy in copies:
        copy.start()
    copies[0].wait()
    wanted[...] = jnp.broadcast_to(requests[...], wanted.shape).T
    copies[1].wait()
    for k in range(NRHS):
        own[pl.ds(k * 16, 16), :] = right_side[pl.ds(k, 16, stride=NRHS), :]
    for copy in copies[2:]:
        copy.wait()


def first_kernel(own, asked, onehot, outgoing):
    lane = lax.broadcasted_iota(jnp.int32, asked.shape, 1)
    hot = (asked[...] == lane).astype(jnp.float32).astype(jnp.bfloat16)
    onehot[...] = hot
    blocks = [own[pl.ds(k * 16, 16), :] for k in range(NRHS)]
    sums = lane_sums({WW * NRHS + k: blocks[k] * blocks[k] for k in range(NRHS)})
    write_outgoing(outgoing, hot, blocks, sums)


def coefficients(rows, system):
    def entry(row, group):
        place = group * NRHS + system
        return jnp.broadcast_to(row[:, place : place + 1], (1, 128))

    beta = jnp.sqrt(entry(rows[0], WW) + EPSILON)
    columns = []
    gram = {}
    for column, row in enumerate(rows[1:]):
        dots = [entry(row, i) for i in range(column + 1)]
        for i in range(column + 1):
            gram[i, column] = gram[column, i] = entry(row, GRAM + i)
        h = []
        for i in range(column + 1):
            value = dots[i]
            for l in range(i):
                value = value - h[l] * gram[l, i]
            h.append(value)
        left = entry(row, WW)
        for i in range(column + 1):
            left = left - h[i] * dots[i]
        for i in range(column + 1):
            residue = dots[i]
            for l in range(column + 1):
                residue = residue - h[l] * gram[l, i]
            left = left - h[i] * residue
        columns.append((h, jnp.sqrt(jnp.maximum(left, 0.0) + EPSILON)))
    return beta, columns


def step_kernel(step, last, *refs):
    refs = list(refs)
    if step == 0:
        count, tiles = refs[:2]
        del refs[:2]
    else:
        weights = refs.pop(0)
    slots, rows_of, onehot, incoming, own = refs[:5]
    del refs[:5]
    earlier_sums = refs[:step]
    del refs[:step]
    earlier = refs[:step]
    del refs[:step]
    basis, sums_out, product, outgoing = refs[:4]
    del refs[:4]
    if step == 0:
        weights = refs.pop(0)
        arrived = refs.pop()
        buffer = refs.pop()
    table, *totals = refs
    devices = onehot.shape[0]
    blocks = 16
    all_blocks = blocks + devices
    stride = NRHS + 1

    if step == 0:
        chunks = tiles.shape[0] // CHUNK
        live = count[0]

        def fetch(chunk):
            slot = lax.rem(chunk, BUFFERS)
            return pltpu.make_async_copy(
                tiles.at[pl.ds(chunk * CHUNK, CHUNK)], buffer.at[slot], arrived.at[slot]
            )

        def pack(chunk):
            slot = lax.rem(chunk, BUFFERS)
            for local in range(CHUNK):
                tile = buffer[slot, local]
                tile = jnp.where(chunk * CHUNK + local < live, tile, 0.0)
                high, low = split2(tile.T)
                pair = chunk * (CHUNK // 2) + local // 2
                lanes = pl.ds((local % 2) * 128, 128)
                weights[pair, pl.ds(0, 128), lanes] = high
                weights[pair, pl.ds(128, 128), lanes] = low

        for chunk in range(BUFFERS - 1):
            fetch(chunk).start()
        fetch(BUFFERS - 1).start()
        fetch(0).wait()
        pack(0)

    sums = jnp.sum(incoming[pl.ds(NRHS, devices, stride=stride), :], axis=0, keepdims=True)
    sums_out[...] = jnp.broadcast_to(sums, (8, 128))
    sums_rows = [ref[pl.ds(0, 1), :] for ref in earlier_sums] + [sums]
    for total in totals:
        total[...] = jnp.zeros_like(total)
    for k in range(NRHS):
        beta, columns = coefficients(sums_rows, k)
        if step == 0:
            scale = 1.0 / beta
            h = []
        else:
            h, length = columns[-1]
            scale = 1.0 / length
        mine = own[pl.ds(k * blocks, blocks), :]
        theirs = incoming[pl.ds(k, devices, stride=stride), :]
        for start, size, value in ((0, blocks, mine), (blocks, devices, theirs)):
            for i in range(step):
                value = value - h[i] * earlier[i][pl.ds(k * all_blocks + start, size), :]
            value = value * scale
            basis[pl.ds(k * all_blocks + start, size), :] = value
            high = value.astype(jnp.bfloat16).astype(jnp.float32)
            table[pl.ds(start * 8 + k, size, stride=8), :] = high
            table[pl.ds(start * 8 + NRHS + k, size, stride=8), :] = value - high

    def multiply(first_pair, size):
        for local in range(size):
            pair = first_pair + local
            picked = [
                table[pl.ds(pl.multiple_of(slots[2 * pair + side] * 8, 8), 8), :]
                for side in range(2)
            ]
            left = jnp.concatenate(picked, axis=0).astype(jnp.bfloat16)
            left = jnp.concatenate([left, left], axis=1)
            result = jnp.dot(left, weights[pair], preferred_element_type=jnp.float32)
            for side in range(2):
                total = totals[(2 * local + side) % TOTALS]
                place = pl.ds(pl.multiple_of(rows_of[2 * pair + side] * 8, 8), 8)
                total[place, :] += result[side * 8 : side * 8 + 8, side * 128 : side * 128 + 128]

    pairs = weights.shape[0]
    if step == 0:
        half = CHUNK // 2

        def body(chunk, carry):
            @pl.when(chunk + BUFFERS - 1 < chunks)
            def _():
                fetch(chunk + BUFFERS - 1).start()

            fetch(chunk).wait()
            pack(chunk)
            multiply((chunk - 1) * half, half)
            return carry

        lax.fori_loop(1, chunks, body, 0)
        multiply((chunks - 1) * half, half)
    else:

        def body(trip, carry):
            multiply(trip * UNROLL, UNROLL)
            return carry

        lax.fori_loop(0, pairs // UNROLL, body, 0)

    total = totals[0]
    summed = total[...]
    for other in totals[1:]:
        summed = summed + other[...]
    total[...] = summed
    new = [
        total[pl.ds(k, blocks, stride=8), :] + total[pl.ds(NRHS + k, blocks, stride=8), :]
        for k in range(NRHS)
    ]
    terms = {}
    for k in range(NRHS):
        product[pl.ds(k * blocks, blocks), :] = new[k]
        latest = basis[pl.ds(k * all_blocks, blocks), :]
        known = [ref[pl.ds(k * all_blocks, blocks), :] for ref in earlier] + [latest]
        for i, vector in enumerate(known):
            terms[i * NRHS + k] = vector * new[k]
            terms[(GRAM + i) * NRHS + k] = vector * latest
        terms[WW * NRHS + k] = new[k] * new[k]
    local = lane_sums(terms)
    if last:
        outgoing[...] = jnp.broadcast_to(local, outgoing.shape)
    else:
        write_outgoing(outgoing, onehot[...], new, local)


def weights_of(beta, columns):
    rotations = []
    triangle = []
    target = [beta]
    for column, (h, length) in enumerate(columns):
        values = list(h) + [length]
        for earlier, (cosine, sine) in enumerate(rotations):
            first, second = values[earlier], values[earlier + 1]
            values[earlier] = cosine * first + sine * second
            values[earlier + 1] = cosine * second - sine * first
        first, second = values[column], values[column + 1]
        radius = jnp.sqrt(first * first + second * second)
        cosine, sine = first / radius, second / radius
        rotations.append((cosine, sine))
        triangle.append(values[:column] + [radius])
        leading = target[column]
        target[column] = cosine * leading
        target.append(-sine * leading)
    size = len(columns)
    weights = [None] * size
    for column in reversed(range(size)):
        value = target[column]
        for later in range(column + 1, size):
            value = value - triangle[later][column] * weights[later]
        weights[column] = value / triangle[column][column]
    return weights


def final_kernel(incoming, sums0, sums1, sums2, basis0, basis1, basis2, solution, hessenberg):
    blocks = 16
    all_blocks = basis0.shape[0] // NRHS
    sums = jnp.sum(incoming[...], axis=0, keepdims=True)
    rows = [ref[pl.ds(0, 1), :] for ref in (sums0, sums1, sums2)] + [sums]
    row_id = lax.broadcasted_iota(jnp.int32, (8, 128), 0)
    lane = lax.broadcasted_iota(jnp.int32, (8, 128), 1)
    tables = [jnp.zeros((8, 128), jnp.float32)] * ITERS
    for k in range(NRHS):
        beta, columns = coefficients(rows, k)
        weights = weights_of(beta, columns)
        value = jnp.zeros((blocks, 128), jnp.float32)
        for weight, basis in zip(weights, (basis0, basis1, basis2)):
            value = value + weight * basis[pl.ds(k * all_blocks, blocks), :]
        solution[pl.ds(k, blocks, stride=NRHS), :] = value
        for column, (h, length) in enumerate(columns):
            for i, entry in enumerate(list(h) + [length]):
                tables[column] = jnp.where((row_id == k) & (lane == i), entry, tables[column])
    for column in range(ITERS):
        hessenberg[column] = tables[column][:NRHS, : ITERS + 1]


def params(limit):
    return pltpu.CompilerParams(vmem_limit_bytes=limit * MIB)


def in_hbm(array):
    return pltpu.with_memory_space_constraint(array, pltpu.HBM)


def exchange(outgoing):
    size = outgoing.shape[0]
    moved = lax.all_to_all(
        outgoing.reshape(size, 1, 128), ROWS, split_axis=0, concat_axis=0, tiled=True
    )
    return moved.reshape(size, 128)


def on_device(tile_values, tile_row, tile_slot, tile_count, requests, right_side):
    devices = lax.axis_size(ROWS)
    tiles = tile_values.shape[0]
    blocks = right_side.shape[0]
    all_blocks = blocks + devices
    f32 = jnp.float32
    flat = right_side.reshape(blocks * NRHS, 128)
    wanted, own, *kept = pl.pallas_call(
        begin_kernel,
        out_shape=(
            jax.ShapeDtypeStruct((devices, 128), jnp.int32),
            jax.ShapeDtypeStruct((blocks * NRHS, 128), f32),
            pltpu.SMEM(tile_slot.shape, tile_slot.dtype),
            pltpu.SMEM(tile_row.shape, tile_row.dtype),
            pltpu.SMEM(tile_count.shape, tile_count.dtype),
        ),
        in_specs=[SMEM] + [HBM] * 4,
        out_specs=(VMEM, VMEM, SMEM, SMEM, SMEM),
        scratch_shapes=[
            pltpu.VMEM((1, devices), jnp.int32),
            pltpu.VMEM(flat.shape, f32),
            pltpu.SemaphoreType.DMA((4,)),
        ],
        compiler_params=params(8),
        name="begin",
    )(tile_count, *map(in_hbm, (requests.reshape(1, devices), flat, tile_slot, tile_row)))
    slots, rows_of, count = kept
    asked = exchange(wanted)
    onehot, outgoing = pl.pallas_call(
        first_kernel,
        out_shape=(
            jax.ShapeDtypeStruct((devices, 128), jnp.bfloat16),
            jax.ShapeDtypeStruct((devices * (NRHS + 1), 128), f32),
        ),
        in_specs=[VMEM, VMEM],
        out_specs=(VMEM, VMEM),
        compiler_params=params(8),
        name="first",
    )(own, asked)
    sums, basis = [], []
    for step in range(ITERS):
        last = step == ITERS - 1
        incoming = exchange(outgoing)
        shapes = [
            jax.ShapeDtypeStruct((NRHS * all_blocks, 128), f32),
            jax.ShapeDtypeStruct((8, 128), f32),
            jax.ShapeDtypeStruct((NRHS * blocks, 128), f32),
            jax.ShapeDtypeStruct((devices if last else devices * (NRHS + 1), 128), f32),
        ]
        scratch = [pltpu.VMEM((all_blocks * 8, 128), f32)]
        scratch += [pltpu.VMEM((blocks * 8, 128), f32)] * TOTALS
        operands = [slots, rows_of, onehot, incoming, own, *sums, *basis]
        specs = [SMEM, SMEM] + [VMEM] * (3 + 2 * step)
        if step == 0:
            shapes.append(pltpu.VMEM((tiles // 2, 256, 256), jnp.bfloat16))
            scratch.append(pltpu.VMEM((BUFFERS, CHUNK, 128, 128), f32))
            scratch.append(pltpu.SemaphoreType.DMA((BUFFERS,)))
            stored = in_hbm(tile_values)
            operands = [count, stored] + operands
            specs = [SMEM, HBM] + specs
        else:
            operands = [weights] + operands
            specs = [VMEM] + specs
        vector, row, own, outgoing, *kept = pl.pallas_call(
            functools.partial(step_kernel, step, last),
            out_shape=shapes,
            in_specs=specs,
            out_specs=[VMEM] * len(shapes),
            scratch_shapes=scratch,
            compiler_params=params(24),
            name=f"step{step}",
        )(*operands)
        if kept:
            weights = kept[0]
        sums.append(row)
        basis.append(vector)
    incoming = exchange(outgoing)
    solution, hessenberg = pl.pallas_call(
        final_kernel,
        out_shape=(
            jax.ShapeDtypeStruct((blocks * NRHS, 128), f32),
            jax.ShapeDtypeStruct((ITERS, NRHS, ITERS + 1), f32),
        ),
        in_specs=[VMEM] * (1 + 2 * ITERS),
        out_specs=(VMEM, VMEM),
        compiler_params=params(8),
        name="final",
    )(incoming, *sums, *basis)
    return solution.reshape(blocks, NRHS, 128), hessenberg.transpose(1, 2, 0)


def solution(mesh):
    finer = Mesh(mesh.devices.reshape(4, 4, 4, 2), ROWS)
    placed = (
        P(ROWS, None, None),
        P(ROWS),
        P(ROWS),
        P(ROWS),
        P(ROWS, None, None),
        P(ROWS, None, None),
    )
    return jax.shard_map(
        on_device,
        mesh=finer,
        in_specs=placed,
        out_specs=(P(ROWS, None, None), P()),
        check_vma=False,
    )
```

```python
import functools

import jax
import jax.numpy as jnp
from jax import lax
from jax.experimental import pallas as pl
from jax.experimental.pallas import tpu as pltpu
from jax.sharding import Mesh
from jax.sharding import PartitionSpec as P

ITERS = 3
NRHS = 4
BLOCKS = 16
STRIDE = NRHS + 1
LEAD = 8
ROWS = ("rows_0", "rows_1", "rows_2", "rows_3")
EPSILON = 1e-06

CHUNK = 26
BUFFERS = 4
TOTALS = 8
MIB = 1 << 20

WW = 3
GRAM = 4

VMEM = pl.BlockSpec(memory_space=pltpu.VMEM)
SMEM = pl.BlockSpec(memory_space=pltpu.SMEM)
HBM = pl.BlockSpec(memory_space=pltpu.HBM)


def row_of(shape=(8, 128)):
    return lax.broadcasted_iota(jnp.int32, shape, 0)


def lane_of(shape=(8, 128)):
    return lax.broadcasted_iota(jnp.int32, shape, 1)


def split2(x):
    high = x.astype(jnp.bfloat16)
    return high, (x - high.astype(jnp.float32)).astype(jnp.bfloat16)


def split3(x):
    first = x.astype(jnp.bfloat16)
    second, third = split2(x - first.astype(jnp.float32))
    return first, second, third


def block(ref, r):
    return ref[pl.ds(8 * r, 8), :]


def in_group(group):
    row, lane = row_of(), lane_of()
    return (lane // NRHS == group) & (lane % NRHS == row % NRHS)


def row_of_sums(terms):
    row = jnp.zeros((8, 128), jnp.float32)
    for group, term in terms.items():
        row = row + jnp.where(in_group(group), jnp.sum(term, axis=1, keepdims=True), 0.0)
    return jnp.sum(jnp.where(row_of() < NRHS, row, 0.0), axis=0, keepdims=True)


def write_outgoing(outgoing, places, blocks, sums):
    low_half = row_of() < NRHS
    packed = [
        jnp.where(low_half, blocks[2 * j], blocks[2 * j + 1]) for j in range(BLOCKS // 2)
    ]
    parts = list(split3(jnp.concatenate(packed, axis=0)))
    row = row_of((64, 128))
    tail = jnp.zeros((64, 128), jnp.float32)
    for place, part in enumerate(split3(sums)):
        tail = jnp.where(row == place, part.astype(jnp.float32), tail)
    parts.append(tail.astype(jnp.bfloat16))
    outgoing[...] = jnp.dot(
        places[...], jnp.concatenate(parts, axis=0), preferred_element_type=jnp.float32
    )


def begin_kernel(*refs):
    count, *given = refs[:5]
    wanted, own, *kept = refs[5:10]
    requests, right_side, copied = refs[10:]
    kept[-1][0] = count[0]
    copies = [
        pltpu.make_async_copy(source, target, copied.at[place])
        for place, (source, target) in enumerate(zip(given, [requests, right_side, *kept[:2]]))
    ]
    for copy in copies:
        copy.start()
    copies[0].wait()
    wanted[...] = jnp.broadcast_to(requests[...], wanted.shape).T
    copies[1].wait()
    low_half = row_of() < NRHS
    for j in range(BLOCKS // 2):
        both = block(right_side, j)
        turned = pltpu.roll(both, NRHS, 0)
        own[pl.ds(16 * j, 8), :] = jnp.where(low_half, both, turned)
        own[pl.ds(16 * j + 8, 8), :] = jnp.where(low_half, turned, both)
    for copy in copies[2:]:
        copy.wait()


def first_kernel(own, asked, places, outgoing):
    f32 = jnp.float32
    devices = asked.shape[0]
    rows = devices * STRIDE
    row = row_of((rows, devices))
    device = STRIDE * lane_of((rows, devices))
    spread = ((row >= device) & (row < device + STRIDE)).astype(f32).astype(jnp.bfloat16)
    ids = asked[...].astype(f32).astype(jnp.bfloat16)
    wanted = jnp.dot(spread, ids, preferred_element_type=f32)
    row = row.astype(f32)
    system = row - STRIDE * jnp.floor(row * (1.0 / STRIDE) + 0.5 / STRIDE)
    lane = lane_of((rows, 128))
    column = (lane % 64).astype(f32)
    own_block = (column == wanted * NRHS + system) & (system < NRHS)
    sums_row = (system >= NRHS) & (lane >= 64) & (lane < 67)
    places[:, :128] = own_block.astype(f32).astype(jnp.bfloat16)
    places[:, 128:] = ((own_block & (lane < 64)) | sums_row).astype(f32).astype(jnp.bfloat16)
    blocks = [block(own, r) for r in range(BLOCKS)]
    sums = row_of_sums({WW: functools.reduce(jnp.add, [b * b for b in blocks])})
    write_outgoing(outgoing, places, blocks, sums)


def coefficients(rows):
    def entry(row, group):
        chosen = jnp.where(in_group(group), row, 0.0)
        return jnp.broadcast_to(jnp.sum(chosen, axis=1, keepdims=True), (8, 128))

    beta = jnp.sqrt(entry(rows[0], WW) + EPSILON)
    columns = []
    gram = {}
    for column, row in enumerate(rows[1:]):
        dots = [entry(row, i) for i in range(column + 1)]
        for i in range(column + 1):
            gram[i, column] = gram[column, i] = entry(row, GRAM + i)
        h = []
        for i in range(column + 1):
            value = dots[i]
            for l in range(i):
                value = value - h[l] * gram[l, i]
            h.append(value)
        left = entry(row, WW)
        for i in range(column + 1):
            left = left - h[i] * dots[i]
        for i in range(column + 1):
            residue = dots[i]
            for l in range(column + 1):
                residue = residue - h[l] * gram[l, i]
            left = left - h[i] * residue
        columns.append((h, jnp.sqrt(jnp.maximum(left, 0.0) + EPSILON)))
    return beta, columns


def strided(values):
    of_system = [jnp.broadcast_to(values[k : k + 1], (8, 128)) for k in range(NRHS)]
    groups = []
    for group in range(STRIDE):
        system = (row_of() + 8 * group) % STRIDE
        chosen = of_system[NRHS - 1]
        for k in range(NRHS - 1):
            chosen = jnp.where(system == k, of_system[k], chosen)
        groups.append(chosen)
    return jnp.concatenate(groups, axis=0)


def step_kernel(step, last, *refs):
    refs = list(refs)

    def take(size):
        taken = refs[:size]
        del refs[:size]
        return taken

    count, tiles = take(2) if step == 0 else (None, None)
    packed = take(2) if step > 0 else None
    slots, rows_of, places, incoming, own = take(5)
    earlier_sums, earlier_own, earlier_halo = take(step), take(step), take(step)
    basis_own, basis_halo, sums_out, product, outgoing = take(5)
    if step == 0:
        packed = take(2)
    (table,) = take(1)
    totals = take(TOTALS)
    devices = incoming.shape[0] // STRIDE
    chunks = packed[0].shape[0] // (CHUNK * 256) * 2

    def fetch(chunk):
        slot = lax.rem(chunk, BUFFERS)
        return pltpu.make_async_copy(
            tiles.at[pl.ds(chunk * CHUNK, CHUNK)], buffer.at[slot], arrived.at[slot]
        )

    def pack(chunk, target, place):
        slot = lax.rem(chunk, BUFFERS)
        for local in range(CHUNK):
            tile = buffer[slot, local]
            tile = jnp.where(chunk * CHUNK + local < live, tile, 0.0)
            high, low = split2(tile.T)
            start = (place * CHUNK + local) * 256
            target[pl.ds(start, 128), :] = high
            target[pl.ds(start + 128, 128), :] = low

    def multiply(chunk, source, place):
        for local in range(CHUNK // 2):
            tile = chunk * CHUNK + 2 * local
            picked = [
                table[pl.ds(pl.multiple_of(slots[tile + side] * 8, 8), 8), :] for side in range(2)
            ]
            left = jnp.concatenate(picked, axis=0).astype(jnp.bfloat16)
            left = jnp.concatenate([left, left], axis=1)
            start = (place * CHUNK + 2 * local) * 256
            right = [source[pl.ds(start + side * 256, 256), :] for side in range(2)]
            result = jnp.dot(
                left, jnp.concatenate(right, axis=1), preferred_element_type=jnp.float32
            )
            for side in range(2):
                total = totals[(2 * local + side) % TOTALS]
                row = pl.ds(pl.multiple_of(rows_of[tile + side] * 8, 8), 8)
                total[row, :] += result[side * 8 : side * 8 + 8, side * 128 : side * 128 + 128]

    if step == 0:
        buffer, arrived = take(2)
        live = count[0]
        for chunk in range(BUFFERS):
            fetch(chunk).start()

    sums = jnp.sum(incoming[pl.ds(NRHS, devices, stride=STRIDE), :], axis=0, keepdims=True)
    sums_out[...] = jnp.broadcast_to(sums, (8, 128))
    beta, columns = coefficients([ref[...] for ref in earlier_sums] + [sums])
    h, length = columns[-1] if step else ([], beta)
    scale = 1.0 / length
    for total in totals:
        total[...] = jnp.zeros_like(total)
    low_half = row_of() < NRHS

    def entry(value):
        high = value.astype(jnp.bfloat16).astype(jnp.float32)
        return jnp.where(low_half, high, value - high)

    for r in range(BLOCKS):
        value = block(own, r)
        for i in range(step):
            value = value - h[i] * block(earlier_own[i], r)
        value = value * scale
        basis_own[pl.ds(8 * r, 8), :] = value
        table[pl.ds(8 * r, 8), :] = entry(value)
    wide_scale = strided(scale)
    wide_h = [strided(value) for value in h]
    period = 8 * STRIDE
    for group in range(devices // 8):
        value = incoming[pl.ds(period * group, period), :]
        rows = pl.ds(LEAD + period * group, period)
        for i in range(step):
            value = value - wide_h[i] * earlier_halo[i][rows, :]
        basis_halo[rows, :] = value * wide_scale
    for device in range(devices):
        start = LEAD + STRIDE * device
        upper = basis_halo[pl.ds(start, 8), :]
        lower = basis_halo[pl.ds(start - NRHS, 8), :]
        table[pl.ds(8 * (BLOCKS + device), 8), :] = entry(jnp.where(low_half, upper, lower))

    if step == 0:
        fetch(0).wait()
        pack(0, packed[0], 0)

        def advance(chunk):
            @pl.when(chunk + BUFFERS - 1 < chunks)
            def _():
                fetch(chunk + BUFFERS - 1).start()

            fetch(chunk).wait()

        def body(trip, carry):
            chunk = 2 * trip + 1
            advance(chunk)
            pack(chunk, packed[1], trip)
            multiply(chunk - 1, packed[0], trip)
            advance(chunk + 1)
            pack(chunk + 1, packed[0], trip + 1)
            multiply(chunk, packed[1], trip)
            return carry

        trips = chunks // 2 - 1
        lax.fori_loop(0, trips, body, 0)
        fetch(chunks - 1).wait()
        pack(chunks - 1, packed[1], trips)
        multiply(chunks - 2, packed[0], trips)
        multiply(chunks - 1, packed[1], trips)
    else:

        def body(trip, carry):
            multiply(2 * trip, packed[0], trip)
            multiply(2 * trip + 1, packed[1], trip)
            return carry

        lax.fori_loop(0, chunks // 2, body, 0)

    blocks = []
    for r in range(BLOCKS):
        value = functools.reduce(jnp.add, [block(total, r) for total in totals])
        value = value + pltpu.roll(value, NRHS, 0)
        product[pl.ds(8 * r, 8), :] = value
        blocks.append(value)
    terms = {WW: functools.reduce(jnp.add, [b * b for b in blocks])}
    for i, vector in enumerate([*earlier_own, basis_own]):
        known = [block(vector, r) for r in range(BLOCKS)]
        latest = [block(basis_own, r) for r in range(BLOCKS)]
        terms[i] = functools.reduce(jnp.add, [a * b for a, b in zip(known, blocks)])
        terms[GRAM + i] = functools.reduce(jnp.add, [a * b for a, b in zip(known, latest)])
    local = row_of_sums(terms)
    if last:
        outgoing[...] = jnp.broadcast_to(local, outgoing.shape)
    else:
        write_outgoing(outgoing, places, blocks, local)


def weights_of(beta, columns):
    rotations = []
    triangle = []
    target = [beta]
    for column, (h, length) in enumerate(columns):
        values = list(h) + [length]
        for earlier, (cosine, sine) in enumerate(rotations):
            first, second = values[earlier], values[earlier + 1]
            values[earlier] = cosine * first + sine * second
            values[earlier + 1] = cosine * second - sine * first
        first, second = values[column], values[column + 1]
        radius = jnp.sqrt(first * first + second * second)
        cosine, sine = first / radius, second / radius
        rotations.append((cosine, sine))
        triangle.append(values[:column] + [radius])
        leading = target[column]
        target[column] = cosine * leading
        target.append(-sine * leading)
    size = len(columns)
    weights = [None] * size
    for column in reversed(range(size)):
        value = target[column]
        for later in range(column + 1, size):
            value = value - triangle[later][column] * weights[later]
        weights[column] = value / triangle[column][column]
    return weights


def final_kernel(incoming, *refs):
    earlier_sums, bases = refs[:ITERS], refs[ITERS : 2 * ITERS]
    solution, hessenberg = refs[2 * ITERS :]
    sums = jnp.sum(incoming[...], axis=0, keepdims=True)
    beta, columns = coefficients([ref[...] for ref in earlier_sums] + [sums])
    weights = weights_of(beta, columns)

    def combined(r):
        value = weights[0] * block(bases[0], r)
        for weight, basis in zip(weights[1:], bases[1:]):
            value = value + weight * block(basis, r)
        return value

    for j in range(BLOCKS // 2):
        both = jnp.where(row_of() < NRHS, combined(2 * j), combined(2 * j + 1))
        solution[pl.ds(8 * j, 8), :] = both
    for column, (h, length) in enumerate(columns):
        table = jnp.zeros((8, 128), jnp.float32)
        for i, value in enumerate([*h, length]):
            table = jnp.where(lane_of() == i, value, table)
        hessenberg[column] = table[:NRHS, : ITERS + 1]


def params(limit):
    return pltpu.CompilerParams(vmem_limit_bytes=limit * MIB)


def in_hbm(array):
    return pltpu.with_memory_space_constraint(array, pltpu.HBM)


def exchange(outgoing):
    size = outgoing.shape[0]
    moved = lax.all_to_all(
        outgoing.reshape(size, 1, 128), ROWS, split_axis=0, concat_axis=0, tiled=True
    )
    return moved.reshape(size, 128)


def on_device(tile_values, tile_row, tile_slot, tile_count, requests, right_side):
    devices = lax.axis_size(ROWS)
    tiles = tile_values.shape[0]
    f32 = jnp.float32
    flat = right_side.reshape(BLOCKS * NRHS, 128)
    block_rows = jax.ShapeDtypeStruct((8 * BLOCKS, 128), f32)
    sum_rows = jax.ShapeDtypeStruct((8, 128), f32)
    message = jax.ShapeDtypeStruct((devices * STRIDE, 128), f32)
    halo_rows = jax.ShapeDtypeStruct((LEAD + devices * STRIDE + 8, 128), f32)
    wanted, own, *kept = pl.pallas_call(
        begin_kernel,
        out_shape=(
            jax.ShapeDtypeStruct((devices, 128), jnp.int32),
            block_rows,
            pltpu.SMEM(tile_slot.shape, tile_slot.dtype),
            pltpu.SMEM(tile_row.shape, tile_row.dtype),
            pltpu.SMEM(tile_count.shape, tile_count.dtype),
        ),
        in_specs=[SMEM] + [HBM] * 4,
        out_specs=(VMEM, VMEM, SMEM, SMEM, SMEM),
        scratch_shapes=[
            pltpu.VMEM((1, devices), jnp.int32),
            pltpu.VMEM(flat.shape, f32),
            pltpu.SemaphoreType.DMA((4,)),
        ],
        compiler_params=params(8),
        name="begin",
    )(tile_count, *map(in_hbm, (requests.reshape(1, devices), flat, tile_slot, tile_row)))
    slots, rows_of, count = kept
    asked = exchange(wanted)
    places, outgoing = pl.pallas_call(
        first_kernel,
        out_shape=(jax.ShapeDtypeStruct((devices * STRIDE, 256), jnp.bfloat16), message),
        in_specs=[VMEM, VMEM],
        out_specs=(VMEM, VMEM),
        compiler_params=params(8),
        name="first",
    )(own, asked)
    sums, owns, halos = [], [], []
    packed = []
    for step in range(ITERS):
        last = step == ITERS - 1
        incoming = exchange(outgoing)
        shapes = [
            block_rows,
            halo_rows,
            sum_rows,
            block_rows,
            jax.ShapeDtypeStruct((devices, 128), f32) if last else message,
        ]
        scratch = [pltpu.VMEM((8 * (BLOCKS + devices), 128), f32)]
        scratch += [pltpu.VMEM(block_rows.shape, f32)] * TOTALS
        operands = [slots, rows_of, places, incoming, own, *sums, *owns, *halos]
        specs = [SMEM, SMEM] + [VMEM] * (len(operands) - 2)
        if step == 0:
            shapes += [pltpu.VMEM((tiles // 2 * 256, 128), jnp.bfloat16)] * 2
            scratch.append(pltpu.VMEM((BUFFERS, CHUNK, 128, 128), f32))
            scratch.append(pltpu.SemaphoreType.DMA((BUFFERS,)))
            operands = [count, in_hbm(tile_values)] + operands
            specs = [SMEM, HBM] + specs
        else:
            operands = packed + operands
            specs = [VMEM, VMEM] + specs
        vector, halo, row, own, outgoing, *kept = pl.pallas_call(
            functools.partial(step_kernel, step, last),
            out_shape=shapes,
            in_specs=specs,
            out_specs=[VMEM] * len(shapes),
            scratch_shapes=scratch,
            compiler_params=params(24),
            name=f"step{step}",
        )(*operands)
        packed = kept or packed
        sums.append(row)
        owns.append(vector)
        halos.append(halo)
    incoming = exchange(outgoing)
    solution, hessenberg = pl.pallas_call(
        final_kernel,
        out_shape=(
            jax.ShapeDtypeStruct(flat.shape, f32),
            jax.ShapeDtypeStruct((ITERS, NRHS, ITERS + 1), f32),
        ),
        in_specs=[VMEM] * (1 + 2 * ITERS),
        out_specs=(VMEM, VMEM),
        compiler_params=params(8),
        name="final",
    )(incoming, *sums, *owns)
    return solution.reshape(right_side.shape), hessenberg.transpose(1, 2, 0)


def solution(mesh):
    finer = Mesh(mesh.devices.reshape(4, 4, 4, 2), ROWS)
    placed = (
        P(ROWS, None, None),
        P(ROWS),
        P(ROWS),
        P(ROWS),
        P(ROWS, None, None),
        P(ROWS, None, None),
    )
    return jax.shard_map(
        on_device,
        mesh=finer,
        in_specs=placed,
        out_specs=(P(ROWS, None, None), P()),
        check_vma=False,
    )
```

```python
import functools

import jax
import jax.numpy as jnp
from jax import lax
from jax.experimental import pallas as pl
from jax.experimental.pallas import tpu as pltpu
from jax.sharding import Mesh
from jax.sharding import PartitionSpec as P

ITERS = 3
NRHS = 4
BLOCKS = 16
STRIDE = NRHS + 1
LEAD = 8
ROWS = ("rows_0", "rows_1", "rows_2", "rows_3")
EPSILON = 1e-06

CHUNK = 26
TOTALS = 8
COVER = 20_000_000_000
MIB = 1 << 20

WW = 3
GRAM = 4

VMEM = pl.BlockSpec(memory_space=pltpu.VMEM)
SMEM = pl.BlockSpec(memory_space=pltpu.SMEM)
HBM = pl.BlockSpec(memory_space=pltpu.HBM)


def row_of(shape=(8, 128)):
    return lax.broadcasted_iota(jnp.int32, shape, 0)


def lane_of(shape=(8, 128)):
    return lax.broadcasted_iota(jnp.int32, shape, 1)


def split2(x):
    high = x.astype(jnp.bfloat16)
    return high, (x - high.astype(jnp.float32)).astype(jnp.bfloat16)


def split3(x):
    first = x.astype(jnp.bfloat16)
    second, third = split2(x - first.astype(jnp.float32))
    return first, second, third


def block(ref, r):
    return ref[pl.ds(8 * r, 8), :]


def in_group(group):
    row, lane = row_of(), lane_of()
    return (lane // NRHS == group) & (lane % NRHS == row % NRHS)


def row_of_sums(terms):
    row = jnp.zeros((8, 128), jnp.float32)
    for group, term in terms.items():
        row = row + jnp.where(in_group(group), jnp.sum(term, axis=1, keepdims=True), 0.0)
    return jnp.sum(jnp.where(row_of() < NRHS, row, 0.0), axis=0, keepdims=True)


def write_outgoing(outgoing, chosen, vector, sums):
    devices = chosen.shape[0]
    systems = [vector[pl.ds(k, BLOCKS, stride=8), :] for k in range(NRHS)]
    parts = jnp.concatenate(split3(jnp.concatenate(systems, axis=1)), axis=0)
    pick = jnp.concatenate([chosen[...][:, :BLOCKS]] * 3, axis=1)
    picked = jnp.dot(pick, parts, preferred_element_type=jnp.float32)
    for k in range(NRHS):
        rows = pl.ds(k, devices, stride=STRIDE)
        outgoing[rows, :] = picked[:, k * 128 : (k + 1) * 128]
    rows = pl.ds(NRHS, devices, stride=STRIDE)
    outgoing[rows, :] = jnp.broadcast_to(sums, (devices, 128))


def begin_kernel(*refs):
    count, *given = refs[:5]
    wanted, own, *kept = refs[5:10]
    requests, right_side, copied = refs[10:]
    kept[-1][0] = count[0]
    copies = [
        pltpu.make_async_copy(source, target, copied.at[place])
        for place, (source, target) in enumerate(zip(given, [requests, right_side, *kept[:2]]))
    ]
    for copy in copies:
        copy.start()
    copies[0].wait()
    wanted[...] = jnp.broadcast_to(requests[...], wanted.shape).T
    copies[1].wait()
    low_half = row_of() < NRHS
    for j in range(BLOCKS // 2):
        both = block(right_side, j)
        turned = pltpu.roll(both, NRHS, 0)
        own[pl.ds(16 * j, 8), :] = jnp.where(low_half, both, turned)
        own[pl.ds(16 * j + 8, 8), :] = jnp.where(low_half, turned, both)
    for copy in copies[2:]:
        copy.wait()


def first_kernel(own, asked, chosen, outgoing):
    hot = asked[...] == lane_of(asked.shape)
    chosen[...] = hot.astype(jnp.float32).astype(jnp.bfloat16)
    blocks = [block(own, r) for r in range(BLOCKS)]
    sums = row_of_sums({WW: functools.reduce(jnp.add, [b * b for b in blocks])})
    write_outgoing(outgoing, chosen, own, sums)


def coefficients(rows):
    def entry(row, group):
        chosen = jnp.where(in_group(group), row, 0.0)
        return jnp.broadcast_to(jnp.sum(chosen, axis=1, keepdims=True), (8, 128))

    beta = jnp.sqrt(entry(rows[0], WW) + EPSILON)
    columns = []
    gram = {}
    for column, row in enumerate(rows[1:]):
        dots = [entry(row, i) for i in range(column + 1)]
        for i in range(column + 1):
            gram[i, column] = gram[column, i] = entry(row, GRAM + i)
        h = []
        for i in range(column + 1):
            value = dots[i]
            for l in range(i):
                value = value - h[l] * gram[l, i]
            h.append(value)
        left = entry(row, WW)
        for i in range(column + 1):
            left = left - h[i] * dots[i]
        for i in range(column + 1):
            residue = dots[i]
            for l in range(column + 1):
                residue = residue - h[l] * gram[l, i]
            left = left - h[i] * residue
        columns.append((h, jnp.sqrt(jnp.maximum(left, 0.0) + EPSILON)))
    return beta, columns


def strided(values):
    of_system = [jnp.broadcast_to(values[k : k + 1], (8, 128)) for k in range(NRHS)]
    groups = []
    for group in range(STRIDE):
        system = (row_of() + 8 * group) % STRIDE
        chosen = of_system[NRHS - 1]
        for k in range(NRHS - 1):
            chosen = jnp.where(system == k, of_system[k], chosen)
        groups.append(chosen)
    return jnp.concatenate(groups, axis=0)


def step_kernel(step, last, *refs):
    refs = list(refs)

    def take(size):
        taken = refs[:size]
        del refs[:size]
        return taken

    count, tiles = take(2) if step == 0 else (None, None)
    packed = take(2) if step > 0 else None
    slots, rows_of, chosen, incoming, own = take(5)
    earlier_sums, earlier_own, earlier_halo = take(step), take(step), take(step)
    basis_own, sums_out, outgoing = take(3)
    if not last:
        basis_halo, product = take(2)
    if step == 0:
        packed = take(2)
    (table,) = take(1)
    totals = take(TOTALS)
    if last:
        basis_halo, product = take(2)
    devices = incoming.shape[0] // STRIDE
    chunks = packed[0].shape[0] // (CHUNK * 256) * 2

    def pack(chunk, target, place):
        for local in range(CHUNK):
            tile = tiles[chunk * CHUNK + local]
            tile = jnp.where(chunk * CHUNK + local < live, tile, 0.0)
            high, low = split2(tile.T)
            start = (place * CHUNK + local) * 256
            target[pl.ds(start, 128), :] = high
            target[pl.ds(start + 128, 128), :] = low

    def multiply(chunk, source, place):
        for local in range(CHUNK // 2):
            tile = chunk * CHUNK + 2 * local
            picked = [
                table[pl.ds(pl.multiple_of(slots[tile + side] * 8, 8), 8), :] for side in range(2)
            ]
            left = jnp.concatenate(picked, axis=0).astype(jnp.bfloat16)
            left = jnp.concatenate([left, left], axis=1)
            start = (place * CHUNK + 2 * local) * 256
            right = [source[pl.ds(start + side * 256, 256), :] for side in range(2)]
            result = jnp.dot(
                left, jnp.concatenate(right, axis=1), preferred_element_type=jnp.float32
            )
            for side in range(2):
                total = totals[(2 * local + side) % TOTALS]
                row = pl.ds(pl.multiple_of(rows_of[tile + side] * 8, 8), 8)
                total[row, :] += result[side * 8 : side * 8 + 8, side * 128 : side * 128 + 128]

    if step == 0:
        live = count[0]

    sums = jnp.sum(incoming[pl.ds(NRHS, devices, stride=STRIDE), :], axis=0, keepdims=True)
    sums_out[...] = jnp.broadcast_to(sums, (8, 128))
    beta, columns = coefficients([ref[...] for ref in earlier_sums] + [sums])
    h, length = columns[-1] if step else ([], beta)
    scale = 1.0 / length
    for total in totals:
        total[...] = jnp.zeros_like(total)
    low_half = row_of() < NRHS

    def entry(value):
        high = value.astype(jnp.bfloat16).astype(jnp.float32)
        return jnp.where(low_half, high, value - high)

    for r in range(BLOCKS):
        value = block(own, r)
        for i in range(step):
            value = value - h[i] * block(earlier_own[i], r)
        value = value * scale
        basis_own[pl.ds(8 * r, 8), :] = value
        table[pl.ds(8 * r, 8), :] = entry(value)
    wide_scale = strided(scale)
    wide_h = [strided(value) for value in h]
    period = 8 * STRIDE
    for group in range(devices // 8):
        value = incoming[pl.ds(period * group, period), :]
        rows = pl.ds(LEAD + period * group, period)
        for i in range(step):
            value = value - wide_h[i] * earlier_halo[i][rows, :]
        basis_halo[rows, :] = value * wide_scale
    for device in range(devices):
        start = LEAD + STRIDE * device
        upper = basis_halo[pl.ds(start, 8), :]
        lower = basis_halo[pl.ds(start - NRHS, 8), :]
        table[pl.ds(8 * (BLOCKS + device), 8), :] = entry(jnp.where(low_half, upper, lower))

    if step == 0:
        pack(0, packed[0], 0)

        def body(trip, carry):
            chunk = 2 * trip + 1
            pack(chunk, packed[1], trip)
            multiply(chunk - 1, packed[0], trip)
            pack(chunk + 1, packed[0], trip + 1)
            multiply(chunk, packed[1], trip)
            return carry

        trips = chunks // 2 - 1
        lax.fori_loop(0, trips, body, 0)
        pack(chunks - 1, packed[1], trips)
        multiply(chunks - 2, packed[0], trips)
        multiply(chunks - 1, packed[1], trips)
    else:

        def body(trip, carry):
            multiply(2 * trip, packed[0], trip)
            multiply(2 * trip + 1, packed[1], trip)
            return carry

        lax.fori_loop(0, chunks // 2, body, 0)

    blocks = []
    for r in range(BLOCKS):
        value = functools.reduce(jnp.add, [block(total, r) for total in totals])
        value = value + pltpu.roll(value, NRHS, 0)
        product[pl.ds(8 * r, 8), :] = value
        blocks.append(value)
    terms = {WW: functools.reduce(jnp.add, [b * b for b in blocks])}
    for i, vector in enumerate([*earlier_own, basis_own]):
        known = [block(vector, r) for r in range(BLOCKS)]
        latest = [block(basis_own, r) for r in range(BLOCKS)]
        terms[i] = functools.reduce(jnp.add, [a * b for a, b in zip(known, blocks)])
        terms[GRAM + i] = functools.reduce(jnp.add, [a * b for a, b in zip(known, latest)])
    local = row_of_sums(terms)
    if last:
        outgoing[...] = jnp.broadcast_to(local, outgoing.shape)
    else:
        write_outgoing(outgoing, chosen, product, local)


def weights_of(beta, columns):
    rotations = []
    triangle = []
    target = [beta]
    for column, (h, length) in enumerate(columns):
        values = list(h) + [length]
        for earlier, (cosine, sine) in enumerate(rotations):
            first, second = values[earlier], values[earlier + 1]
            values[earlier] = cosine * first + sine * second
            values[earlier + 1] = cosine * second - sine * first
        first, second = values[column], values[column + 1]
        radius = jnp.sqrt(first * first + second * second)
        cosine, sine = first / radius, second / radius
        rotations.append((cosine, sine))
        triangle.append(values[:column] + [radius])
        leading = target[column]
        target[column] = cosine * leading
        target.append(-sine * leading)
    size = len(columns)
    weights = [None] * size
    for column in reversed(range(size)):
        value = target[column]
        for later in range(column + 1, size):
            value = value - triangle[later][column] * weights[later]
        weights[column] = value / triangle[column][column]
    return weights


def final_kernel(incoming, *refs):
    earlier_sums, bases = refs[:ITERS], refs[ITERS : 2 * ITERS]
    solution, hessenberg = refs[2 * ITERS :]
    sums = jnp.sum(incoming[...], axis=0, keepdims=True)
    beta, columns = coefficients([ref[...] for ref in earlier_sums] + [sums])
    weights = weights_of(beta, columns)

    def combined(r):
        value = weights[0] * block(bases[0], r)
        for weight, basis in zip(weights[1:], bases[1:]):
            value = value + weight * block(basis, r)
        return value

    for j in range(BLOCKS // 2):
        both = jnp.where(row_of() < NRHS, combined(2 * j), combined(2 * j + 1))
        solution[pl.ds(8 * j, 8), :] = both
    for column, (h, length) in enumerate(columns):
        table = jnp.zeros((8, 128), jnp.float32)
        for i, value in enumerate([*h, length]):
            table = jnp.where(lane_of() == i, value, table)
        hessenberg[column] = table[:NRHS, : ITERS + 1]


def params(limit):
    return pltpu.CompilerParams(vmem_limit_bytes=limit * MIB)


def in_hbm(array):
    return pltpu.with_memory_space_constraint(array, pltpu.HBM)


def exchange(outgoing):
    size = outgoing.shape[0]
    moved = lax.all_to_all(
        outgoing.reshape(size, 1, 128), ROWS, split_axis=0, concat_axis=0, tiled=True
    )
    return moved.reshape(size, 128)


def on_device(tile_values, tile_row, tile_slot, tile_count, requests, right_side):
    devices = lax.axis_size(ROWS)
    tiles = tile_values.shape[0]
    f32 = jnp.float32
    flat = right_side.reshape(BLOCKS * NRHS, 128)
    block_rows = jax.ShapeDtypeStruct((8 * BLOCKS, 128), f32)
    sum_rows = jax.ShapeDtypeStruct((8, 128), f32)
    message = jax.ShapeDtypeStruct((devices * STRIDE, 128), f32)
    halo_rows = jax.ShapeDtypeStruct((LEAD + devices * STRIDE + 8, 128), f32)
    wanted, own, *kept = pl.pallas_call(
        begin_kernel,
        out_shape=(
            jax.ShapeDtypeStruct((devices, 128), jnp.int32),
            block_rows,
            pltpu.SMEM(tile_slot.shape, tile_slot.dtype),
            pltpu.SMEM(tile_row.shape, tile_row.dtype),
            pltpu.SMEM(tile_count.shape, tile_count.dtype),
        ),
        in_specs=[SMEM] + [HBM] * 4,
        out_specs=(VMEM, VMEM, SMEM, SMEM, SMEM),
        scratch_shapes=[
            pltpu.VMEM((1, devices), jnp.int32),
            pltpu.VMEM(flat.shape, f32),
            pltpu.SemaphoreType.DMA((4,)),
        ],
        compiler_params=params(8),
        name="begin",
    )(tile_count, *map(in_hbm, (requests.reshape(1, devices), flat, tile_slot, tile_row)))
    slots, rows_of, count = kept
    asked = exchange(wanted)
    chosen, outgoing = pl.pallas_call(
        first_kernel,
        out_shape=(jax.ShapeDtypeStruct((devices, devices), jnp.bfloat16), message),
        in_specs=[VMEM, VMEM],
        out_specs=(VMEM, VMEM),
        compiler_params=params(8),
        cost_estimate=pl.CostEstimate(flops=COVER, bytes_accessed=0, transcendentals=0),
        name="first",
    )(own, asked)
    sums, owns, halos = [], [], []
    packed = []
    for step in range(ITERS):
        last = step == ITERS - 1
        incoming = exchange(outgoing)
        shapes = [block_rows, sum_rows]
        shapes += [jax.ShapeDtypeStruct((devices, 128), f32)] if last else [message]
        shapes += [] if last else [halo_rows, block_rows]
        scratch = [pltpu.VMEM((8 * (BLOCKS + devices), 128), f32)]
        scratch += [pltpu.VMEM(block_rows.shape, f32)] * TOTALS
        if last:
            scratch += [pltpu.VMEM(halo_rows.shape, f32), pltpu.VMEM(block_rows.shape, f32)]
        operands = [slots, rows_of, chosen, incoming, own, *sums, *owns, *halos]
        specs = [SMEM, SMEM] + [VMEM] * (len(operands) - 2)
        if step == 0:
            shapes += [pltpu.VMEM((tiles // 2 * 256, 128), jnp.bfloat16)] * 2
            operands = [count, tile_values] + operands
            specs = [SMEM, VMEM] + specs
        else:
            operands = packed + operands
            specs = [VMEM, VMEM] + specs
        vector, row, outgoing, *kept = pl.pallas_call(
            functools.partial(step_kernel, step, last),
            out_shape=shapes,
            in_specs=specs,
            out_specs=[VMEM] * len(shapes),
            scratch_shapes=scratch,
            compiler_params=params(20),
            name=f"step{step}",
        )(*operands)
        sums.append(row)
        owns.append(vector)
        if not last:
            halo, own, *packed = [*kept, *packed]
            halos.append(halo)
    incoming = exchange(outgoing)
    solution, hessenberg = pl.pallas_call(
        final_kernel,
        out_shape=(
            jax.ShapeDtypeStruct(flat.shape, f32),
            jax.ShapeDtypeStruct((ITERS, NRHS, ITERS + 1), f32),
        ),
        in_specs=[VMEM] * (1 + 2 * ITERS),
        out_specs=(VMEM, VMEM),
        compiler_params=params(8),
        name="final",
    )(incoming, *sums, *owns)
    return solution.reshape(right_side.shape), hessenberg.transpose(1, 2, 0)


def solution(mesh):
    finer = Mesh(mesh.devices.reshape(4, 4, 4, 2), ROWS)
    placed = (
        P(ROWS, None, None),
        P(ROWS),
        P(ROWS),
        P(ROWS),
        P(ROWS, None, None),
        P(ROWS, None, None),
    )
    return jax.shard_map(
        on_device,
        mesh=finer,
        in_specs=placed,
        out_specs=(P(ROWS, None, None), P()),
        check_vma=False,
    )
```

```python
import functools

import jax
import jax.numpy as jnp
from jax import lax
from jax.experimental import pallas as pl
from jax.experimental.pallas import tpu as pltpu
from jax.sharding import Mesh
from jax.sharding import PartitionSpec as P

ITERS = 3
NRHS = 4
BLOCKS = 16
STRIDE = NRHS + 1
LEAD = 8
ROWS = ("rows_0", "rows_1", "rows_2", "rows_3")
EPSILON = 1e-06

CHUNK = 26
TOTALS = 8
COVER = 20_000_000_000
MIB = 1 << 20

WW = 3
GRAM = 4
NORM = 16

VMEM = pl.BlockSpec(memory_space=pltpu.VMEM)
SMEM = pl.BlockSpec(memory_space=pltpu.SMEM)
HBM = pl.BlockSpec(memory_space=pltpu.HBM)


def row_of(shape=(8, 128)):
    return lax.broadcasted_iota(jnp.int32, shape, 0)


def lane_of(shape=(8, 128)):
    return lax.broadcasted_iota(jnp.int32, shape, 1)


def split2(x):
    high = x.astype(jnp.bfloat16)
    return high, (x - high.astype(jnp.float32)).astype(jnp.bfloat16)


def split3(x):
    first = x.astype(jnp.bfloat16)
    second, third = split2(x - first.astype(jnp.float32))
    return first, second, third


def block(ref, r):
    return ref[pl.ds(8 * r, 8), :]


def in_group(group):
    row, lane = row_of(), lane_of()
    return (lane // NRHS == group) & (lane % NRHS == row % NRHS)


def row_of_sums(terms):
    row = jnp.zeros((8, 128), jnp.float32)
    for group, term in terms.items():
        row = row + jnp.where(in_group(group), jnp.sum(term, axis=1, keepdims=True), 0.0)
    return jnp.sum(jnp.where(row_of() < NRHS, row, 0.0), axis=0, keepdims=True)


def write_outgoing(outgoing, chosen, vector, sums=None):
    devices = chosen.shape[0]
    stride = outgoing.shape[0] // devices
    systems = [vector[pl.ds(k, BLOCKS, stride=8), :] for k in range(NRHS)]
    parts = jnp.concatenate(split3(jnp.concatenate(systems, axis=1)), axis=0)
    pick = jnp.concatenate([chosen[...][:, :BLOCKS]] * 3, axis=1)
    picked = jnp.dot(pick, parts, preferred_element_type=jnp.float32)
    for k in range(NRHS):
        rows = pl.ds(k, devices, stride=stride)
        outgoing[rows, :] = picked[:, k * 128 : (k + 1) * 128]
    if sums is not None:
        rows = pl.ds(NRHS, devices, stride=stride)
        outgoing[rows, :] = jnp.broadcast_to(sums, (devices, 128))


def begin_kernel(*refs):
    count, *given = refs[:5]
    wanted, own, *kept = refs[5:10]
    requests, right_side, copied = refs[10:]
    kept[-1][0] = count[0]
    copies = [
        pltpu.make_async_copy(source, target, copied.at[place])
        for place, (source, target) in enumerate(zip(given, [requests, right_side, *kept[:2]]))
    ]
    for copy in copies:
        copy.start()
    copies[1].wait()
    low_half = row_of() < NRHS
    squares = jnp.zeros((8, 128), jnp.float32)
    for j in range(BLOCKS // 2):
        both = block(right_side, j)
        turned = pltpu.roll(both, NRHS, 0)
        own[pl.ds(16 * j, 8), :] = jnp.where(low_half, both, turned)
        own[pl.ds(16 * j + 8, 8), :] = jnp.where(low_half, turned, both)
        squares = squares + both * both
    sums = row_of_sums({NORM: squares + pltpu.roll(squares, NRHS, 0)})
    copies[0].wait()
    ids = jnp.broadcast_to(requests[...], wanted.shape).T.astype(jnp.float32)
    is_norm = lane_of(wanted.shape) // NRHS == NORM
    wanted[...] = jnp.where(is_norm, jnp.broadcast_to(sums, wanted.shape), ids)
    for copy in copies[2:]:
        copy.wait()


def first_kernel(own, asked, chosen, sums, outgoing):
    hot = asked[...] == lane_of(asked.shape).astype(jnp.float32)
    chosen[...] = hot.astype(jnp.float32).astype(jnp.bfloat16)
    sums[...] = jnp.broadcast_to(jnp.sum(asked[...], axis=0, keepdims=True), sums.shape)
    write_outgoing(outgoing, chosen, own)


def coefficients(rows):
    def entry(row, group):
        chosen = jnp.where(in_group(group), row, 0.0)
        return jnp.broadcast_to(jnp.sum(chosen, axis=1, keepdims=True), (8, 128))

    beta = jnp.sqrt(entry(rows[0], NORM) + EPSILON)
    columns = []
    gram = {}
    for column, row in enumerate(rows[1:]):
        dots = [entry(row, i) for i in range(column + 1)]
        for i in range(column + 1):
            gram[i, column] = gram[column, i] = entry(row, GRAM + i)
        h = []
        for i in range(column + 1):
            value = dots[i]
            for l in range(i):
                value = value - h[l] * gram[l, i]
            h.append(value)
        left = entry(row, WW)
        for i in range(column + 1):
            left = left - h[i] * dots[i]
        for i in range(column + 1):
            residue = dots[i]
            for l in range(column + 1):
                residue = residue - h[l] * gram[l, i]
            left = left - h[i] * residue
        columns.append((h, jnp.sqrt(jnp.maximum(left, 0.0) + EPSILON)))
    return beta, columns


def strided(values):
    of_system = [jnp.broadcast_to(values[k : k + 1], (8, 128)) for k in range(NRHS)]
    groups = []
    for group in range(STRIDE):
        system = (row_of() + 8 * group) % STRIDE
        chosen = of_system[NRHS - 1]
        for k in range(NRHS - 1):
            chosen = jnp.where(system == k, of_system[k], chosen)
        groups.append(chosen)
    return jnp.concatenate(groups, axis=0)


def step_kernel(step, last, *refs):
    refs = list(refs)

    def take(size):
        taken = refs[:size]
        del refs[:size]
        return taken

    count, tiles = take(2) if step == 0 else (None, None)
    packed = take(2) if step > 0 else None
    slots, rows_of, chosen, incoming, own = take(5)
    earlier_sums, earlier_own, earlier_halo = take(max(step, 1)), take(step), take(step)
    basis_own, outgoing = take(2)
    if step > 0:
        (sums_out,) = take(1)
    if not last:
        basis_halo, product = take(2)
    if step == 0:
        packed = take(2)
    (table,) = take(1)
    totals = take(TOTALS)
    if last:
        basis_halo, product = take(2)
    devices = table.shape[0] // 8 - BLOCKS
    chunks = sum(part.shape[0] for part in packed) // (CHUNK * 256)

    def pack(tile_id, target, start):
        tile = jnp.where(tile_id < live, tiles[tile_id], 0.0)
        high, low = split2(tile.T)
        both = jnp.concatenate([high, low], axis=0)
        target[pl.ds(start, 256), :] = both
        return both

    def multiply(chunk, source, place, fresh=False):
        for local in range(CHUNK // 2):
            tile = chunk * CHUNK + 2 * local
            picked = [
                table[pl.ds(pl.multiple_of(slots[tile + side] * 8, 8), 8), :] for side in range(2)
            ]
            left = jnp.concatenate(picked, axis=0).astype(jnp.bfloat16)
            left = jnp.concatenate([left, left], axis=1)
            start = (place * CHUNK + 2 * local) * 256
            if fresh:
                right = [pack(tile + side, source, start + side * 256) for side in range(2)]
            else:
                right = [source[pl.ds(start + side * 256, 256), :] for side in range(2)]
            result = jnp.dot(
                left, jnp.concatenate(right, axis=1), preferred_element_type=jnp.float32
            )
            for side in range(2):
                total = totals[(2 * local + side) % TOTALS]
                row = pl.ds(pl.multiple_of(rows_of[tile + side] * 8, 8), 8)
                total[row, :] += result[side * 8 : side * 8 + 8, side * 128 : side * 128 + 128]

    if step == 0:
        live = count[0]

    sums_rows = [ref[...] for ref in earlier_sums]
    if step > 0:
        rows = pl.ds(NRHS, devices, stride=STRIDE)
        sums_rows.append(jnp.sum(incoming[rows, :], axis=0, keepdims=True))
        sums_out[...] = jnp.broadcast_to(sums_rows[-1], (8, 128))
    beta, columns = coefficients(sums_rows)
    h, length = columns[-1] if step else ([], beta)
    scale = 1.0 / length
    for total in totals:
        total[...] = jnp.zeros_like(total)
    low_half = row_of() < NRHS

    def entry(value):
        high = value.astype(jnp.bfloat16).astype(jnp.float32)
        return jnp.where(low_half, high, value - high)

    for r in range(BLOCKS):
        value = block(own, r)
        for i in range(step):
            value = value - h[i] * block(earlier_own[i], r)
        value = value * scale
        basis_own[pl.ds(8 * r, 8), :] = value
        table[pl.ds(8 * r, 8), :] = entry(value)
    if step == 0:
        for j in range(devices // 2):
            both = block(incoming, j) * scale
            turned = pltpu.roll(both, NRHS, 0)
            for side in range(2):
                value = jnp.where(low_half, turned, both) if side else jnp.where(low_half, both, turned)
                device = 2 * j + side
                basis_halo[pl.ds(LEAD + STRIDE * device, 8), :] = value
                table[pl.ds(8 * (BLOCKS + device), 8), :] = entry(value)
    else:
        wide_scale = strided(scale)
        wide_h = [strided(value) for value in h]
        period = 8 * STRIDE
        for group in range(devices // 8):
            value = incoming[pl.ds(period * group, period), :]
            rows = pl.ds(LEAD + period * group, period)
            for i in range(step):
                value = value - wide_h[i] * earlier_halo[i][rows, :]
            basis_halo[rows, :] = value * wide_scale
        for device in range(devices):
            start = LEAD + STRIDE * device
            upper = basis_halo[pl.ds(start, 8), :]
            lower = basis_halo[pl.ds(start - NRHS, 8), :]
            table[pl.ds(8 * (BLOCKS + device), 8), :] = entry(jnp.where(low_half, upper, lower))

    if step == 0:
        def body(trip, carry):
            multiply(2 * trip, packed[0], trip, True)
            multiply(2 * trip + 1, packed[1], trip, True)
            return carry

        lax.fori_loop(0, chunks // 2, body, 0)
    else:
        for chunk in range(chunks):
            multiply(chunk, packed[chunk % 2], chunk // 2)

    blocks = []
    for r in range(BLOCKS):
        value = functools.reduce(jnp.add, [block(total, r) for total in totals])
        value = value + pltpu.roll(value, NRHS, 0)
        product[pl.ds(8 * r, 8), :] = value
        blocks.append(value)
    terms = {WW: functools.reduce(jnp.add, [b * b for b in blocks])}
    for i, vector in enumerate([*earlier_own, basis_own]):
        known = [block(vector, r) for r in range(BLOCKS)]
        latest = [block(basis_own, r) for r in range(BLOCKS)]
        terms[i] = functools.reduce(jnp.add, [a * b for a, b in zip(known, blocks)])
        terms[GRAM + i] = functools.reduce(jnp.add, [a * b for a, b in zip(known, latest)])
    local = row_of_sums(terms)
    if last:
        outgoing[...] = jnp.broadcast_to(local, outgoing.shape)
    else:
        write_outgoing(outgoing, chosen, product, local)


def weights_of(beta, columns):
    rotations = []
    triangle = []
    target = [beta]
    for column, (h, length) in enumerate(columns):
        values = list(h) + [length]
        for earlier, (cosine, sine) in enumerate(rotations):
            first, second = values[earlier], values[earlier + 1]
            values[earlier] = cosine * first + sine * second
            values[earlier + 1] = cosine * second - sine * first
        first, second = values[column], values[column + 1]
        radius = jnp.sqrt(first * first + second * second)
        cosine, sine = first / radius, second / radius
        rotations.append((cosine, sine))
        triangle.append(values[:column] + [radius])
        leading = target[column]
        target[column] = cosine * leading
        target.append(-sine * leading)
    size = len(columns)
    weights = [None] * size
    for column in reversed(range(size)):
        value = target[column]
        for later in range(column + 1, size):
            value = value - triangle[later][column] * weights[later]
        weights[column] = value / triangle[column][column]
    return weights


def final_kernel(incoming, *refs):
    earlier_sums, bases = refs[:ITERS], refs[ITERS : 2 * ITERS]
    solution, hessenberg = refs[2 * ITERS :]
    sums = jnp.sum(incoming[...], axis=0, keepdims=True)
    beta, columns = coefficients([ref[...] for ref in earlier_sums] + [sums])
    weights = weights_of(beta, columns)

    def combined(r):
        value = weights[0] * block(bases[0], r)
        for weight, basis in zip(weights[1:], bases[1:]):
            value = value + weight * block(basis, r)
        return value

    for j in range(BLOCKS // 2):
        both = jnp.where(row_of() < NRHS, combined(2 * j), combined(2 * j + 1))
        solution[pl.ds(8 * j, 8), :] = both
    for column, (h, length) in enumerate(columns):
        table = jnp.zeros((8, 128), jnp.float32)
        for i, value in enumerate([*h, length]):
            table = jnp.where(lane_of() == i, value, table)
        hessenberg[column] = table[:NRHS, : ITERS + 1]


def params(limit):
    return pltpu.CompilerParams(vmem_limit_bytes=limit * MIB)


def in_hbm(array):
    return pltpu.with_memory_space_constraint(array, pltpu.HBM)


def exchange(outgoing):
    size = outgoing.shape[0]
    moved = lax.all_to_all(
        outgoing.reshape(size, 1, 128), ROWS, split_axis=0, concat_axis=0, tiled=True
    )
    return moved.reshape(size, 128)


def on_device(tile_values, tile_row, tile_slot, tile_count, requests, right_side):
    devices = lax.axis_size(ROWS)
    tiles = tile_values.shape[0]
    f32 = jnp.float32
    flat = right_side.reshape(BLOCKS * NRHS, 128)
    block_rows = jax.ShapeDtypeStruct((8 * BLOCKS, 128), f32)
    sum_rows = jax.ShapeDtypeStruct((8, 128), f32)
    message = jax.ShapeDtypeStruct((devices * STRIDE, 128), f32)
    halo_rows = jax.ShapeDtypeStruct((LEAD + devices * STRIDE + 8, 128), f32)
    wanted, own, *kept = pl.pallas_call(
        begin_kernel,
        out_shape=(
            jax.ShapeDtypeStruct((devices, 128), f32),
            block_rows,
            pltpu.SMEM(tile_slot.shape, tile_slot.dtype),
            pltpu.SMEM(tile_row.shape, tile_row.dtype),
            pltpu.SMEM(tile_count.shape, tile_count.dtype),
        ),
        in_specs=[SMEM] + [HBM] * 4,
        out_specs=(VMEM, VMEM, SMEM, SMEM, SMEM),
        scratch_shapes=[
            pltpu.VMEM((1, devices), jnp.int32),
            pltpu.VMEM(flat.shape, f32),
            pltpu.SemaphoreType.DMA((4,)),
        ],
        compiler_params=params(8),
        name="begin",
    )(tile_count, *map(in_hbm, (requests.reshape(1, devices), flat, tile_slot, tile_row)))
    slots, rows_of, count = kept
    asked = exchange(wanted)
    chosen, norms, outgoing = pl.pallas_call(
        first_kernel,
        out_shape=(
            jax.ShapeDtypeStruct((devices, devices), jnp.bfloat16),
            sum_rows,
            jax.ShapeDtypeStruct((devices * NRHS, 128), f32),
        ),
        in_specs=[VMEM, VMEM],
        out_specs=(VMEM, VMEM, VMEM),
        compiler_params=params(8),
        cost_estimate=pl.CostEstimate(flops=COVER, bytes_accessed=0, transcendentals=0),
        name="first",
    )(own, asked)
    sums, owns, halos = [norms], [], []
    packed = []
    for step in range(ITERS):
        last = step == ITERS - 1
        incoming = exchange(outgoing)
        shapes = [block_rows]
        shapes += [jax.ShapeDtypeStruct((devices, 128), f32)] if last else [message]
        shapes += [sum_rows] if step > 0 else []
        shapes += [] if last else [halo_rows, block_rows]
        scratch = [pltpu.VMEM((8 * (BLOCKS + devices), 128), f32)]
        scratch += [pltpu.VMEM(block_rows.shape, f32)] * TOTALS
        if last:
            scratch += [pltpu.VMEM(halo_rows.shape, f32), pltpu.VMEM(block_rows.shape, f32)]
        operands = [slots, rows_of, chosen, incoming, own, *sums, *owns, *halos]
        specs = [SMEM, SMEM] + [VMEM] * (len(operands) - 2)
        if step == 0:
            odd = tiles // CHUNK // 2 * CHUNK
            shapes += [
                pltpu.VMEM((part * 256, 128), jnp.bfloat16) for part in (tiles - odd, odd)
            ]
            operands = [count, tile_values] + operands
            specs = [SMEM, VMEM] + specs
        else:
            operands = packed + operands
            specs = [VMEM, VMEM] + specs
        vector, outgoing, *kept = pl.pallas_call(
            functools.partial(step_kernel, step, last),
            out_shape=shapes,
            in_specs=specs,
            out_specs=[VMEM] * len(shapes),
            scratch_shapes=scratch,
            compiler_params=params(20),
            name=f"step{step}",
        )(*operands)
        if step > 0:
            sums.append(kept.pop(0))
        owns.append(vector)
        if not last:
            halo, own, *packed = [*kept, *packed]
            halos.append(halo)
    incoming = exchange(outgoing)
    solution, hessenberg = pl.pallas_call(
        final_kernel,
        out_shape=(
            jax.ShapeDtypeStruct(flat.shape, f32),
            jax.ShapeDtypeStruct((ITERS, NRHS, ITERS + 1), f32),
        ),
        in_specs=[VMEM] * (1 + 2 * ITERS),
        out_specs=(VMEM, VMEM),
        compiler_params=params(8),
        name="final",
    )(incoming, *sums, *owns)
    return solution.reshape(right_side.shape), hessenberg.transpose(1, 2, 0)


def solution(mesh):
    finer = Mesh(mesh.devices.reshape(4, 4, 4, 2), ROWS)
    placed = (
        P(ROWS, None, None),
        P(ROWS),
        P(ROWS),
        P(ROWS),
        P(ROWS, None, None),
        P(ROWS, None, None),
    )
    return jax.shard_map(
        on_device,
        mesh=finer,
        in_specs=placed,
        out_specs=(P(ROWS, None, None), P()),
        check_vma=False,
    )
```

```python
import functools

import jax
import jax.numpy as jnp
from jax import lax
from jax.experimental import pallas as pl
from jax.experimental.pallas import tpu as pltpu
from jax.sharding import Mesh
from jax.sharding import PartitionSpec as P

ITERS = 3
NRHS = 4
BLOCKS = 16
STRIDE = NRHS + 1
LEAD = 8
ROWS = ("rows_0", "rows_1", "rows_2", "rows_3")
EPSILON = 1e-06

CHUNK = 104
TOTALS = 8
TURNED = 4
COVER = 20_000_000_000
MIB = 1 << 20

WW = 3
GRAM = 4
NORM = 16

VMEM = pl.BlockSpec(memory_space=pltpu.VMEM)
SMEM = pl.BlockSpec(memory_space=pltpu.SMEM)
HBM = pl.BlockSpec(memory_space=pltpu.HBM)


def row_of(shape=(8, 128)):
    return lax.broadcasted_iota(jnp.int32, shape, 0)


def lane_of(shape=(8, 128)):
    return lax.broadcasted_iota(jnp.int32, shape, 1)


def split2(x):
    high = x.astype(jnp.bfloat16)
    return high, (x - high.astype(jnp.float32)).astype(jnp.bfloat16)


def split3(x):
    first = x.astype(jnp.bfloat16)
    second, third = split2(x - first.astype(jnp.float32))
    return first, second, third


def block(ref, r):
    return ref[pl.ds(8 * r, 8), :]


def in_group(group):
    row, lane = row_of(), lane_of()
    return (lane // NRHS == group) & (lane % NRHS == row % NRHS)


def row_of_sums(terms):
    row = jnp.zeros((8, 128), jnp.float32)
    for group, term in terms.items():
        row = row + jnp.where(in_group(group), jnp.sum(term, axis=1, keepdims=True), 0.0)
    return jnp.sum(jnp.where(row_of() < NRHS, row, 0.0), axis=0, keepdims=True)


def write_outgoing(outgoing, chosen, vector, sums=None):
    devices = chosen.shape[0]
    stride = outgoing.shape[0] // devices
    systems = [vector[pl.ds(k, BLOCKS, stride=8), :] for k in range(NRHS)]
    parts = jnp.concatenate(split3(jnp.concatenate(systems, axis=1)), axis=0)
    pick = jnp.concatenate([chosen[...][:, :BLOCKS]] * 3, axis=1)
    picked = jnp.dot(pick, parts, preferred_element_type=jnp.float32)
    for k in range(NRHS):
        rows = pl.ds(k, devices, stride=stride)
        outgoing[rows, :] = picked[:, k * 128 : (k + 1) * 128]
    if sums is not None:
        rows = pl.ds(NRHS, devices, stride=stride)
        outgoing[rows, :] = jnp.broadcast_to(sums, (devices, 128))


def begin_kernel(*refs):
    count, *given = refs[:5]
    wanted, own, *kept = refs[5:10]
    requests, right_side, copied = refs[10:]
    kept[-1][0] = count[0]
    copies = [
        pltpu.make_async_copy(source, target, copied.at[place])
        for place, (source, target) in enumerate(zip(given, [requests, right_side, *kept[:2]]))
    ]
    for copy in copies:
        copy.start()
    copies[0].wait()
    copies[1].wait()
    low_half = row_of() < NRHS
    squares = jnp.zeros((8, 128), jnp.float32)
    for j in range(BLOCKS // 2):
        both = block(right_side, j)
        turned = pltpu.roll(both, NRHS, 0)
        own[pl.ds(16 * j, 8), :] = jnp.where(low_half, both, turned)
        own[pl.ds(16 * j + 8, 8), :] = jnp.where(low_half, turned, both)
        squares = squares + both * both
    sums = row_of_sums({NORM: squares + pltpu.roll(squares, NRHS, 0)})
    ids = jnp.broadcast_to(requests[...], wanted.shape).T.astype(jnp.float32)
    is_norm = lane_of(wanted.shape) // NRHS == NORM
    wanted[...] = jnp.where(is_norm, jnp.broadcast_to(sums, wanted.shape), ids)
    for copy in copies[2:]:
        copy.wait()


def first_kernel(own, asked, chosen, sums, outgoing):
    hot = asked[...] == lane_of(asked.shape).astype(jnp.float32)
    chosen[...] = hot.astype(jnp.float32).astype(jnp.bfloat16)
    sums[...] = jnp.broadcast_to(jnp.sum(asked[...], axis=0, keepdims=True), sums.shape)
    write_outgoing(outgoing, chosen, own)


def coefficients(rows):
    def entry(row, group):
        chosen = jnp.where(in_group(group), row, 0.0)
        return jnp.broadcast_to(jnp.sum(chosen, axis=1, keepdims=True), (8, 128))

    beta = jnp.sqrt(entry(rows[0], NORM) + EPSILON)
    columns = []
    gram = {}
    for column, row in enumerate(rows[1:]):
        dots = [entry(row, i) for i in range(column + 1)]
        for i in range(column + 1):
            gram[i, column] = gram[column, i] = entry(row, GRAM + i)
        h = []
        for i in range(column + 1):
            value = dots[i]
            for l in range(i):
                value = value - h[l] * gram[l, i]
            h.append(value)
        left = entry(row, WW)
        for i in range(column + 1):
            left = left - h[i] * dots[i]
        for i in range(column + 1):
            residue = dots[i]
            for l in range(column + 1):
                residue = residue - h[l] * gram[l, i]
            left = left - h[i] * residue
        columns.append((h, jnp.sqrt(jnp.maximum(left, 0.0) + EPSILON)))
    return beta, columns


def strided(values):
    of_system = [jnp.broadcast_to(values[k : k + 1], (8, 128)) for k in range(NRHS)]
    groups = []
    for group in range(STRIDE):
        system = (row_of() + 8 * group) % STRIDE
        chosen = of_system[NRHS - 1]
        for k in range(NRHS - 1):
            chosen = jnp.where(system == k, of_system[k], chosen)
        groups.append(chosen)
    return jnp.concatenate(groups, axis=0)


def step_kernel(step, last, *refs):
    refs = list(refs)

    def take(size):
        taken = refs[:size]
        del refs[:size]
        return taken

    count, tiles = take(2) if step == 0 else (None, None)
    packed = take(2) if step > 0 else None
    slots, rows_of, chosen, incoming, own = take(5)
    earlier_sums, earlier_own, earlier_halo = take(max(step, 1)), take(step), take(step)
    basis_own, outgoing = take(2)
    if step > 0:
        (sums_out,) = take(1)
    if not last:
        basis_halo, product = take(2)
    if step == 0:
        packed = take(2)
    (table,) = take(1)
    totals = take(TOTALS)
    if last:
        basis_halo, product = take(2)
    devices = table.shape[0] // 8 - BLOCKS
    chunks = sum(part.shape[0] for part in packed) // (CHUNK * 256)

    def pack(tile_id, target, start):
        tile = jnp.where(tile_id < live, tiles[tile_id], 0.0)
        high, low = split2(tile.T)
        both = jnp.concatenate([high, low], axis=0)
        target[pl.ds(start, 256), :] = both
        return both

    def turn(left, tile_id, target, start):
        sides = [jnp.where(tile_id + side < live, tiles[tile_id + side], 0.0) for side in range(2)]
        right = jnp.concatenate([jnp.concatenate(split2(tile), axis=1) for tile in sides], axis=0)
        result = lax.dot_general(
            jnp.concatenate([left, identity[...]], axis=0),
            right,
            (((1,), (1,)), ((), ())),
            preferred_element_type=jnp.float32,
        )
        turned = result[16:].astype(jnp.bfloat16)
        target[pl.ds(start, 256), :] = turned[:, :128]
        target[pl.ds(start + 256, 256), :] = turned[:, 128:]
        return result[:16]

    def multiply(chunk, source, place, fresh=False):
        for local in range(CHUNK // 2):
            tile = chunk * CHUNK + 2 * local
            picked = [
                table[pl.ds(pl.multiple_of(slots[tile + side] * 8, 8), 8), :] for side in range(2)
            ]
            left = jnp.concatenate(picked, axis=0).astype(jnp.bfloat16)
            left = jnp.concatenate([left, left], axis=1)
            start = (place * CHUNK + 2 * local) * 256
            if fresh and local % TURNED == 0:
                result = turn(left, tile, source, start)
            elif fresh:
                right = [pack(tile + side, source, start + side * 256) for side in range(2)]
            else:
                right = [source[pl.ds(start + side * 256, 256), :] for side in range(2)]
            if not (fresh and local % TURNED == 0):
                result = jnp.dot(
                    left, jnp.concatenate(right, axis=1), preferred_element_type=jnp.float32
                )
            for side in range(2):
                total = totals[(2 * local + side) % TOTALS]
                row = pl.ds(pl.multiple_of(rows_of[tile + side] * 8, 8), 8)
                total[row, :] += result[side * 8 : side * 8 + 8, side * 128 : side * 128 + 128]

    if step == 0:
        live = count[0]
        (identity,) = take(1)
        diagonal = row_of((256, 256)) == lane_of((256, 256))
        identity[...] = diagonal.astype(jnp.float32).astype(jnp.bfloat16)

    sums_rows = [ref[...] for ref in earlier_sums]
    if step > 0:
        rows = pl.ds(NRHS, devices, stride=STRIDE)
        sums_rows.append(jnp.sum(incoming[rows, :], axis=0, keepdims=True))
        sums_out[...] = jnp.broadcast_to(sums_rows[-1], (8, 128))
    beta, columns = coefficients(sums_rows)
    h, length = columns[-1] if step else ([], beta)
    scale = 1.0 / length
    for total in totals:
        total[...] = jnp.zeros_like(total)
    low_half = row_of() < NRHS

    def entry(value):
        high = value.astype(jnp.bfloat16).astype(jnp.float32)
        return jnp.where(low_half, high, value - high)

    for r in range(BLOCKS):
        value = block(own, r)
        for i in range(step):
            value = value - h[i] * block(earlier_own[i], r)
        value = value * scale
        basis_own[pl.ds(8 * r, 8), :] = value
        table[pl.ds(8 * r, 8), :] = entry(value)
    if step == 0:
        for j in range(devices // 2):
            both = block(incoming, j) * scale
            turned = pltpu.roll(both, NRHS, 0)
            for side in range(2):
                value = jnp.where(low_half, turned, both) if side else jnp.where(low_half, both, turned)
                device = 2 * j + side
                basis_halo[pl.ds(LEAD + STRIDE * device, 8), :] = value
                table[pl.ds(8 * (BLOCKS + device), 8), :] = entry(value)
    else:
        wide_scale = strided(scale)
        wide_h = [strided(value) for value in h]
        period = 8 * STRIDE
        for group in range(devices // 8):
            value = incoming[pl.ds(period * group, period), :]
            rows = pl.ds(LEAD + period * group, period)
            for i in range(step):
                value = value - wide_h[i] * earlier_halo[i][rows, :]
            basis_halo[rows, :] = value * wide_scale
        for device in range(devices):
            start = LEAD + STRIDE * device
            upper = basis_halo[pl.ds(start, 8), :]
            lower = basis_halo[pl.ds(start - NRHS, 8), :]
            table[pl.ds(8 * (BLOCKS + device), 8), :] = entry(jnp.where(low_half, upper, lower))

    if step == 0:
        def body(trip, carry):
            multiply(2 * trip, packed[0], trip, True)
            multiply(2 * trip + 1, packed[1], trip, True)
            return carry

        lax.fori_loop(0, chunks // 2, body, 0)
    else:
        for chunk in range(chunks):
            multiply(chunk, packed[chunk % 2], chunk // 2)

    blocks = []
    for r in range(BLOCKS):
        value = functools.reduce(jnp.add, [block(total, r) for total in totals])
        value = value + pltpu.roll(value, NRHS, 0)
        product[pl.ds(8 * r, 8), :] = value
        blocks.append(value)
    terms = {WW: functools.reduce(jnp.add, [b * b for b in blocks])}
    for i, vector in enumerate([*earlier_own, basis_own]):
        known = [block(vector, r) for r in range(BLOCKS)]
        latest = [block(basis_own, r) for r in range(BLOCKS)]
        terms[i] = functools.reduce(jnp.add, [a * b for a, b in zip(known, blocks)])
        terms[GRAM + i] = functools.reduce(jnp.add, [a * b for a, b in zip(known, latest)])
    local = row_of_sums(terms)
    if last:
        outgoing[...] = jnp.broadcast_to(local, outgoing.shape)
    else:
        write_outgoing(outgoing, chosen, product, local)


def weights_of(beta, columns):
    rotations = []
    triangle = []
    target = [beta]
    for column, (h, length) in enumerate(columns):
        values = list(h) + [length]
        for earlier, (cosine, sine) in enumerate(rotations):
            first, second = values[earlier], values[earlier + 1]
            values[earlier] = cosine * first + sine * second
            values[earlier + 1] = cosine * second - sine * first
        first, second = values[column], values[column + 1]
        radius = jnp.sqrt(first * first + second * second)
        cosine, sine = first / radius, second / radius
        rotations.append((cosine, sine))
        triangle.append(values[:column] + [radius])
        leading = target[column]
        target[column] = cosine * leading
        target.append(-sine * leading)
    size = len(columns)
    weights = [None] * size
    for column in reversed(range(size)):
        value = target[column]
        for later in range(column + 1, size):
            value = value - triangle[later][column] * weights[later]
        weights[column] = value / triangle[column][column]
    return weights


def final_kernel(incoming, *refs):
    earlier_sums, bases = refs[:ITERS], refs[ITERS : 2 * ITERS]
    solution, hessenberg = refs[2 * ITERS :]
    sums = jnp.sum(incoming[...], axis=0, keepdims=True)
    beta, columns = coefficients([ref[...] for ref in earlier_sums] + [sums])
    weights = weights_of(beta, columns)

    def combined(r):
        value = weights[0] * block(bases[0], r)
        for weight, basis in zip(weights[1:], bases[1:]):
            value = value + weight * block(basis, r)
        return value

    for j in range(BLOCKS // 2):
        both = jnp.where(row_of() < NRHS, combined(2 * j), combined(2 * j + 1))
        solution[pl.ds(8 * j, 8), :] = both
    for column, (h, length) in enumerate(columns):
        table = jnp.zeros((8, 128), jnp.float32)
        for i, value in enumerate([*h, length]):
            table = jnp.where(lane_of() == i, value, table)
        hessenberg[column] = table[:NRHS, : ITERS + 1]


def params(limit):
    return pltpu.CompilerParams(vmem_limit_bytes=limit * MIB)


def in_hbm(array):
    return pltpu.with_memory_space_constraint(array, pltpu.HBM)


def exchange(outgoing):
    size = outgoing.shape[0]
    moved = lax.all_to_all(
        outgoing.reshape(size, 1, 128), ROWS, split_axis=0, concat_axis=0, tiled=True
    )
    return moved.reshape(size, 128)


def on_device(tile_values, tile_row, tile_slot, tile_count, requests, right_side):
    devices = lax.axis_size(ROWS)
    tiles = tile_values.shape[0]
    f32 = jnp.float32
    flat = right_side.reshape(BLOCKS * NRHS, 128)
    block_rows = jax.ShapeDtypeStruct((8 * BLOCKS, 128), f32)
    sum_rows = jax.ShapeDtypeStruct((8, 128), f32)
    message = jax.ShapeDtypeStruct((devices * STRIDE, 128), f32)
    halo_rows = jax.ShapeDtypeStruct((LEAD + devices * STRIDE + 8, 128), f32)
    wanted, own, *kept = pl.pallas_call(
        begin_kernel,
        out_shape=(
            jax.ShapeDtypeStruct((devices, 128), f32),
            block_rows,
            pltpu.SMEM(tile_slot.shape, tile_slot.dtype),
            pltpu.SMEM(tile_row.shape, tile_row.dtype),
            pltpu.SMEM(tile_count.shape, tile_count.dtype),
        ),
        in_specs=[SMEM] + [HBM] * 4,
        out_specs=(VMEM, VMEM, SMEM, SMEM, SMEM),
        scratch_shapes=[
            pltpu.VMEM((1, devices), jnp.int32),
            pltpu.VMEM(flat.shape, f32),
            pltpu.SemaphoreType.DMA((4,)),
        ],
        compiler_params=params(8),
        name="begin",
    )(tile_count, *map(in_hbm, (requests.reshape(1, devices), flat, tile_slot, tile_row)))
    slots, rows_of, count = kept
    asked = exchange(wanted)
    chosen, norms, outgoing = pl.pallas_call(
        first_kernel,
        out_shape=(
            jax.ShapeDtypeStruct((devices, devices), jnp.bfloat16),
            sum_rows,
            jax.ShapeDtypeStruct((devices * NRHS, 128), f32),
        ),
        in_specs=[VMEM, VMEM],
        out_specs=(VMEM, VMEM, VMEM),
        compiler_params=params(8),
        cost_estimate=pl.CostEstimate(flops=COVER, bytes_accessed=0, transcendentals=0),
        name="first",
    )(own, asked)
    sums, owns, halos = [norms], [], []
    packed = []
    for step in range(ITERS):
        last = step == ITERS - 1
        incoming = exchange(outgoing)
        shapes = [block_rows]
        shapes += [jax.ShapeDtypeStruct((devices, 128), f32)] if last else [message]
        shapes += [sum_rows] if step > 0 else []
        shapes += [] if last else [halo_rows, block_rows]
        scratch = [pltpu.VMEM((8 * (BLOCKS + devices), 128), f32)]
        scratch += [pltpu.VMEM(block_rows.shape, f32)] * TOTALS
        if last:
            scratch += [pltpu.VMEM(halo_rows.shape, f32), pltpu.VMEM(block_rows.shape, f32)]
        operands = [slots, rows_of, chosen, incoming, own, *sums, *owns, *halos]
        specs = [SMEM, SMEM] + [VMEM] * (len(operands) - 2)
        if step == 0:
            odd = tiles // CHUNK // 2 * CHUNK
            scratch.append(pltpu.VMEM((256, 256), jnp.bfloat16))
            shapes += [
                pltpu.VMEM((part * 256, 128), jnp.bfloat16) for part in (tiles - odd, odd)
            ]
            operands = [count, tile_values] + operands
            specs = [SMEM, VMEM] + specs
        else:
            operands = packed + operands
            specs = [VMEM, VMEM] + specs
        vector, outgoing, *kept = pl.pallas_call(
            functools.partial(step_kernel, step, last),
            out_shape=shapes,
            in_specs=specs,
            out_specs=[VMEM] * len(shapes),
            scratch_shapes=scratch,
            compiler_params=params(20),
            name=f"step{step}",
        )(*operands)
        if step > 0:
            sums.append(kept.pop(0))
        owns.append(vector)
        if not last:
            halo, own, *packed = [*kept, *packed]
            halos.append(halo)
    incoming = exchange(outgoing)
    solution, hessenberg = pl.pallas_call(
        final_kernel,
        out_shape=(
            jax.ShapeDtypeStruct(flat.shape, f32),
            jax.ShapeDtypeStruct((ITERS, NRHS, ITERS + 1), f32),
        ),
        in_specs=[VMEM] * (1 + 2 * ITERS),
        out_specs=(VMEM, VMEM),
        compiler_params=params(8),
        name="final",
    )(incoming, *sums, *owns)
    return solution.reshape(right_side.shape), hessenberg.transpose(1, 2, 0)


def solution(mesh):
    finer = Mesh(mesh.devices.reshape(4, 4, 4, 2), ROWS)
    placed = (
        P(ROWS, None, None),
        P(ROWS),
        P(ROWS),
        P(ROWS),
        P(ROWS, None, None),
        P(ROWS, None, None),
    )
    return jax.shard_map(
        on_device,
        mesh=finer,
        in_specs=placed,
        out_specs=(P(ROWS, None, None), P()),
        check_vma=False,
    )
```

```python
import functools

import jax
import jax.numpy as jnp
from jax import lax
from jax.experimental import pallas as pl
from jax.experimental.pallas import tpu as pltpu
from jax.sharding import Mesh
from jax.sharding import PartitionSpec as P

ITERS = 3
NRHS = 4
BLOCKS = 16
STRIDE = NRHS + 1
LEAD = 8
ROWS = ("rows_0", "rows_1", "rows_2", "rows_3")
EPSILON = 1e-06

TOTALS = 4
TURNED = 4
COVER = 20_000_000_000
MIB = 1 << 20

WW = 3
GRAM = 4
NORM = 16

VMEM = pl.BlockSpec(memory_space=pltpu.VMEM)
SMEM = pl.BlockSpec(memory_space=pltpu.SMEM)
HBM = pl.BlockSpec(memory_space=pltpu.HBM)


def row_of(shape=(8, 128)):
    return lax.broadcasted_iota(jnp.int32, shape, 0)


def lane_of(shape=(8, 128)):
    return lax.broadcasted_iota(jnp.int32, shape, 1)


def split2(x):
    high = x.astype(jnp.bfloat16)
    return high, (x - high.astype(jnp.float32)).astype(jnp.bfloat16)


def split3(x):
    first = x.astype(jnp.bfloat16)
    second, third = split2(x - first.astype(jnp.float32))
    return first, second, third


def block(ref, r):
    return ref[pl.ds(8 * r, 8), :]


def in_group(group):
    row, lane = row_of(), lane_of()
    return (lane // NRHS == group) & (lane % NRHS == row % NRHS)


def row_of_sums(terms):
    row = jnp.zeros((8, 128), jnp.float32)
    for group, term in terms.items():
        row = row + jnp.where(in_group(group), jnp.sum(term, axis=1, keepdims=True), 0.0)
    return jnp.sum(jnp.where(row_of() < NRHS, row, 0.0), axis=0, keepdims=True)


def write_outgoing(outgoing, chosen, vector, sums=None):
    devices = chosen.shape[0]
    stride = outgoing.shape[0] // devices
    systems = [vector[pl.ds(k, BLOCKS, stride=8), :] for k in range(NRHS)]
    parts = jnp.concatenate(split3(jnp.concatenate(systems, axis=1)), axis=0)
    pick = jnp.concatenate([chosen[...][:, :BLOCKS]] * 3, axis=1)
    picked = jnp.dot(pick, parts, preferred_element_type=jnp.float32)
    for k in range(NRHS):
        rows = pl.ds(k, devices, stride=stride)
        outgoing[rows, :] = picked[:, k * 128 : (k + 1) * 128]
    if sums is not None:
        rows = pl.ds(NRHS, devices, stride=stride)
        outgoing[rows, :] = jnp.broadcast_to(sums, (devices, 128))


def begin_kernel(*refs):
    count, *given = refs[:5]
    wanted, own, *kept = refs[5:10]
    requests, right_side, copied = refs[10:]
    kept[-1][0] = count[0]
    copies = [
        pltpu.make_async_copy(source, target, copied.at[place])
        for place, (source, target) in enumerate(zip(given, [requests, right_side, *kept[:2]]))
    ]
    for copy in copies:
        copy.start()
    copies[0].wait()
    copies[1].wait()
    low_half = row_of() < NRHS
    squares = jnp.zeros((8, 128), jnp.float32)
    for j in range(BLOCKS // 2):
        both = block(right_side, j)
        turned = pltpu.roll(both, NRHS, 0)
        own[pl.ds(16 * j, 8), :] = jnp.where(low_half, both, turned)
        own[pl.ds(16 * j + 8, 8), :] = jnp.where(low_half, turned, both)
        squares = squares + both * both
    sums = row_of_sums({NORM: squares + pltpu.roll(squares, NRHS, 0)})
    ids = jnp.broadcast_to(requests[...], wanted.shape).T.astype(jnp.float32)
    is_norm = lane_of(wanted.shape) // NRHS == NORM
    wanted[...] = jnp.where(is_norm, jnp.broadcast_to(sums, wanted.shape), ids)
    for copy in copies[2:]:
        copy.wait()


def first_kernel(own, asked, chosen, sums, outgoing):
    hot = asked[...] == lane_of(asked.shape).astype(jnp.float32)
    chosen[...] = hot.astype(jnp.float32).astype(jnp.bfloat16)
    sums[...] = jnp.broadcast_to(jnp.sum(asked[...], axis=0, keepdims=True), sums.shape)
    write_outgoing(outgoing, chosen, own)


def coefficients(rows):
    def entry(row, group):
        chosen = jnp.where(in_group(group), row, 0.0)
        return jnp.broadcast_to(jnp.sum(chosen, axis=1, keepdims=True), (8, 128))

    beta = jnp.sqrt(entry(rows[0], NORM) + EPSILON)
    columns = []
    gram = {}
    for column, row in enumerate(rows[1:]):
        dots = [entry(row, i) for i in range(column + 1)]
        for i in range(column + 1):
            gram[i, column] = gram[column, i] = entry(row, GRAM + i)
        h = []
        for i in range(column + 1):
            value = dots[i]
            for l in range(i):
                value = value - h[l] * gram[l, i]
            h.append(value)
        left = entry(row, WW)
        for i in range(column + 1):
            left = left - h[i] * dots[i]
        for i in range(column + 1):
            residue = dots[i]
            for l in range(column + 1):
                residue = residue - h[l] * gram[l, i]
            left = left - h[i] * residue
        columns.append((h, jnp.sqrt(jnp.maximum(left, 0.0) + EPSILON)))
    return beta, columns


def strided(values):
    of_system = [jnp.broadcast_to(values[k : k + 1], (8, 128)) for k in range(NRHS)]
    groups = []
    for group in range(STRIDE):
        system = (row_of() + 8 * group) % STRIDE
        chosen = of_system[NRHS - 1]
        for k in range(NRHS - 1):
            chosen = jnp.where(system == k, of_system[k], chosen)
        groups.append(chosen)
    return jnp.concatenate(groups, axis=0)


def step_kernel(step, last, *refs):
    refs = list(refs)

    def take(size):
        taken = refs[:size]
        del refs[:size]
        return taken

    count, tiles = take(2) if step == 0 else (None, None)
    packed = refs.pop(0) if step > 0 else None
    slots, rows_of, chosen, incoming, own = take(5)
    earlier_sums, earlier_own, earlier_halo = take(max(step, 1)), take(step), take(step)
    basis_own, outgoing = take(2)
    if step > 0:
        (sums_out,) = take(1)
    if not last:
        basis_halo, product = take(2)
    if step == 0:
        packed = refs.pop(0)
    (table,) = take(1)
    totals = take(TOTALS)
    if last:
        basis_halo, product = take(2)
    devices = table.shape[0] // 8 - BLOCKS

    def pack(tile_id, target, start):
        tile = jnp.where(tile_id < live, tiles[tile_id], 0.0)
        high, low = split2(tile.T)
        both = jnp.concatenate([high, low], axis=0)
        target[pl.ds(start, 256), :] = both
        return both

    def turn(left, tile_id, target, start):
        sides = [jnp.where(tile_id + side < live, tiles[tile_id + side], 0.0) for side in range(2)]
        right = jnp.concatenate([jnp.concatenate(split2(tile), axis=1) for tile in sides], axis=0)
        result = lax.dot_general(
            jnp.concatenate([left, identity[...]], axis=0),
            right,
            (((1,), (1,)), ((), ())),
            preferred_element_type=jnp.float32,
        )
        turned = result[16:].astype(jnp.bfloat16)
        target[pl.ds(start, 256), :] = turned[:, :128]
        target[pl.ds(start + 256, 256), :] = turned[:, 128:]
        return result[:16]

    def multiply(tile):
        own_slots = BLOCKS + devices
        picked = [
            table[pl.ds(8 * tile if tile < own_slots else pl.multiple_of(slots[tile] * 8, 8), 8), :]
            for tile in (tile, tile + 1)
        ]
        left = jnp.concatenate(picked, axis=0).astype(jnp.bfloat16)
        left = jnp.concatenate([left, left], axis=1)
        start = tile * 256
        if step == 0 and tile // 2 % TURNED == 0:
            result = turn(left, tile, packed, start)
        else:
            if step == 0:
                right = [pack(tile + side, packed, start + side * 256) for side in range(2)]
            else:
                right = [packed[pl.ds(start + side * 256, 256), :] for side in range(2)]
            result = jnp.dot(
                left, jnp.concatenate(right, axis=1), preferred_element_type=jnp.float32
            )
        for side in range(2):
            total = totals[(tile + side) % TOTALS]
            row = tile + side
            row = 8 * row if row < BLOCKS else pl.multiple_of(rows_of[row] * 8, 8)
            part = result[side * 8 : side * 8 + 8, side * 128 : side * 128 + 128]
            total[pl.ds(row, 8), :] += part

    if step == 0:
        live = count[0]
        (identity,) = take(1)
        diagonal = row_of((256, 256)) == lane_of((256, 256))
        identity[...] = diagonal.astype(jnp.float32).astype(jnp.bfloat16)

    sums_rows = [ref[...] for ref in earlier_sums]
    if step > 0:
        rows = pl.ds(NRHS, devices, stride=STRIDE)
        sums_rows.append(jnp.sum(incoming[rows, :], axis=0, keepdims=True))
        sums_out[...] = jnp.broadcast_to(sums_rows[-1], (8, 128))
    beta, columns = coefficients(sums_rows)
    h, length = columns[-1] if step else ([], beta)
    scale = 1.0 / length
    for total in totals:
        total[...] = jnp.zeros_like(total)
    low_half = row_of() < NRHS

    def entry(value):
        high = value.astype(jnp.bfloat16).astype(jnp.float32)
        return jnp.where(low_half, high, value - high)

    for r in range(BLOCKS):
        value = block(own, r)
        for i in range(step):
            value = value - h[i] * block(earlier_own[i], r)
        value = value * scale
        basis_own[pl.ds(8 * r, 8), :] = value
        table[pl.ds(8 * r, 8), :] = entry(value)
    if step == 0:
        for j in range(devices // 2):
            both = block(incoming, j) * scale
            turned = pltpu.roll(both, NRHS, 0)
            for side in range(2):
                value = jnp.where(low_half, turned, both) if side else jnp.where(low_half, both, turned)
                device = 2 * j + side
                basis_halo[pl.ds(LEAD + STRIDE * device, 8), :] = value
                table[pl.ds(8 * (BLOCKS + device), 8), :] = entry(value)
    else:
        wide_scale = strided(scale)
        wide_h = [strided(value) for value in h]
        period = 8 * STRIDE
        for group in range(devices // 8):
            value = incoming[pl.ds(period * group, period), :]
            rows = pl.ds(LEAD + period * group, period)
            for i in range(step):
                value = value - wide_h[i] * earlier_halo[i][rows, :]
            basis_halo[rows, :] = value * wide_scale
        for device in range(devices):
            start = LEAD + STRIDE * device
            upper = basis_halo[pl.ds(start, 8), :]
            lower = basis_halo[pl.ds(start - NRHS, 8), :]
            table[pl.ds(8 * (BLOCKS + device), 8), :] = entry(jnp.where(low_half, upper, lower))

    for tile in range(0, packed.shape[0] // 256, 2):
        multiply(tile)

    blocks = []
    for r in range(BLOCKS):
        value = functools.reduce(jnp.add, [block(total, r) for total in totals])
        value = value + pltpu.roll(value, NRHS, 0)
        product[pl.ds(8 * r, 8), :] = value
        blocks.append(value)
    terms = {WW: functools.reduce(jnp.add, [b * b for b in blocks])}
    for i, vector in enumerate([*earlier_own, basis_own]):
        known = [block(vector, r) for r in range(BLOCKS)]
        latest = [block(basis_own, r) for r in range(BLOCKS)]
        terms[i] = functools.reduce(jnp.add, [a * b for a, b in zip(known, blocks)])
        terms[GRAM + i] = functools.reduce(jnp.add, [a * b for a, b in zip(known, latest)])
    local = row_of_sums(terms)
    if last:
        outgoing[...] = jnp.broadcast_to(local, outgoing.shape)
    else:
        write_outgoing(outgoing, chosen, product, local)


def weights_of(beta, columns):
    rotations = []
    triangle = []
    target = [beta]
    for column, (h, length) in enumerate(columns):
        values = list(h) + [length]
        for earlier, (cosine, sine) in enumerate(rotations):
            first, second = values[earlier], values[earlier + 1]
            values[earlier] = cosine * first + sine * second
            values[earlier + 1] = cosine * second - sine * first
        first, second = values[column], values[column + 1]
        radius = jnp.sqrt(first * first + second * second)
        cosine, sine = first / radius, second / radius
        rotations.append((cosine, sine))
        triangle.append(values[:column] + [radius])
        leading = target[column]
        target[column] = cosine * leading
        target.append(-sine * leading)
    size = len(columns)
    weights = [None] * size
    for column in reversed(range(size)):
        value = target[column]
        for later in range(column + 1, size):
            value = value - triangle[later][column] * weights[later]
        weights[column] = value / triangle[column][column]
    return weights


def final_kernel(incoming, *refs):
    earlier_sums, bases = refs[:ITERS], refs[ITERS : 2 * ITERS]
    solution, hessenberg = refs[2 * ITERS :]
    sums = jnp.sum(incoming[...], axis=0, keepdims=True)
    beta, columns = coefficients([ref[...] for ref in earlier_sums] + [sums])
    weights = weights_of(beta, columns)

    def combined(r):
        value = weights[0] * block(bases[0], r)
        for weight, basis in zip(weights[1:], bases[1:]):
            value = value + weight * block(basis, r)
        return value

    for j in range(BLOCKS // 2):
        both = jnp.where(row_of() < NRHS, combined(2 * j), combined(2 * j + 1))
        solution[pl.ds(8 * j, 8), :] = both
    for column, (h, length) in enumerate(columns):
        table = jnp.zeros((8, 128), jnp.float32)
        for i, value in enumerate([*h, length]):
            table = jnp.where(lane_of() == i, value, table)
        hessenberg[column] = table[:NRHS, : ITERS + 1]


def params(limit):
    return pltpu.CompilerParams(vmem_limit_bytes=limit * MIB)


def in_hbm(array):
    return pltpu.with_memory_space_constraint(array, pltpu.HBM)


def exchange(outgoing):
    size = outgoing.shape[0]
    moved = lax.all_to_all(
        outgoing.reshape(size, 1, 128), ROWS, split_axis=0, concat_axis=0, tiled=True
    )
    return moved.reshape(size, 128)


def on_device(tile_values, tile_row, tile_slot, tile_count, requests, right_side):
    devices = lax.axis_size(ROWS)
    tiles = tile_values.shape[0]
    f32 = jnp.float32
    flat = right_side.reshape(BLOCKS * NRHS, 128)
    block_rows = jax.ShapeDtypeStruct((8 * BLOCKS, 128), f32)
    sum_rows = jax.ShapeDtypeStruct((8, 128), f32)
    message = jax.ShapeDtypeStruct((devices * STRIDE, 128), f32)
    halo_rows = jax.ShapeDtypeStruct((LEAD + devices * STRIDE + 8, 128), f32)
    wanted, own, *kept = pl.pallas_call(
        begin_kernel,
        out_shape=(
            jax.ShapeDtypeStruct((devices, 128), f32),
            block_rows,
            pltpu.SMEM(tile_slot.shape, tile_slot.dtype),
            pltpu.SMEM(tile_row.shape, tile_row.dtype),
            pltpu.SMEM(tile_count.shape, tile_count.dtype),
        ),
        in_specs=[SMEM] + [HBM] * 4,
        out_specs=(VMEM, VMEM, SMEM, SMEM, SMEM),
        scratch_shapes=[
            pltpu.VMEM((1, devices), jnp.int32),
            pltpu.VMEM(flat.shape, f32),
            pltpu.SemaphoreType.DMA((4,)),
        ],
        compiler_params=params(8),
        name="begin",
    )(tile_count, *map(in_hbm, (requests.reshape(1, devices), flat, tile_slot, tile_row)))
    slots, rows_of, count = kept
    asked = exchange(wanted)
    chosen, norms, outgoing = pl.pallas_call(
        first_kernel,
        out_shape=(
            jax.ShapeDtypeStruct((devices, devices), jnp.bfloat16),
            sum_rows,
            jax.ShapeDtypeStruct((devices * NRHS, 128), f32),
        ),
        in_specs=[VMEM, VMEM],
        out_specs=(VMEM, VMEM, VMEM),
        compiler_params=params(8),
        cost_estimate=pl.CostEstimate(flops=COVER, bytes_accessed=0, transcendentals=0),
        name="first",
    )(own, asked)
    sums, owns, halos = [norms], [], []
    packed = None
    for step in range(ITERS):
        last = step == ITERS - 1
        incoming = exchange(outgoing)
        shapes = [block_rows]
        shapes += [jax.ShapeDtypeStruct((devices, 128), f32)] if last else [message]
        shapes += [sum_rows] if step > 0 else []
        shapes += [] if last else [halo_rows, block_rows]
        scratch = [pltpu.VMEM((8 * (BLOCKS + devices), 128), f32)]
        scratch += [pltpu.VMEM(block_rows.shape, f32)] * TOTALS
        if last:
            scratch += [pltpu.VMEM(halo_rows.shape, f32), pltpu.VMEM(block_rows.shape, f32)]
        operands = [slots, rows_of, chosen, incoming, own, *sums, *owns, *halos]
        specs = [SMEM, SMEM] + [VMEM] * (len(operands) - 2)
        if step == 0:
            scratch.append(pltpu.VMEM((256, 256), jnp.bfloat16))
            shapes.append(pltpu.VMEM((tiles * 256, 128), jnp.bfloat16))
            operands = [count, tile_values] + operands
            specs = [SMEM, VMEM] + specs
        else:
            operands = [packed] + operands
            specs = [VMEM] + specs
        vector, outgoing, *kept = pl.pallas_call(
            functools.partial(step_kernel, step, last),
            out_shape=shapes,
            in_specs=specs,
            out_specs=[VMEM] * len(shapes),
            scratch_shapes=scratch,
            compiler_params=params(20),
            name=f"step{step}",
        )(*operands)
        if step > 0:
            sums.append(kept.pop(0))
        owns.append(vector)
        if not last:
            halo, own, *rest = kept
            halos.append(halo)
            packed = rest[0] if step == 0 else packed
    incoming = exchange(outgoing)
    solution, hessenberg = pl.pallas_call(
        final_kernel,
        out_shape=(
            jax.ShapeDtypeStruct(flat.shape, f32),
            jax.ShapeDtypeStruct((ITERS, NRHS, ITERS + 1), f32),
        ),
        in_specs=[VMEM] * (1 + 2 * ITERS),
        out_specs=(VMEM, VMEM),
        compiler_params=params(8),
        name="final",
    )(incoming, *sums, *owns)
    return solution.reshape(right_side.shape), hessenberg.transpose(1, 2, 0)


def solution(mesh):
    finer = Mesh(mesh.devices.reshape(4, 4, 4, 2), ROWS)
    placed = (
        P(ROWS, None, None),
        P(ROWS),
        P(ROWS),
        P(ROWS),
        P(ROWS, None, None),
        P(ROWS, None, None),
    )
    return jax.shard_map(
        on_device,
        mesh=finer,
        in_specs=placed,
        out_specs=(P(ROWS, None, None), P()),
        check_vma=False,
    )
```

```python
import functools

import jax
import jax.numpy as jnp
from jax import lax
from jax.experimental import pallas as pl
from jax.experimental.pallas import tpu as pltpu
from jax.sharding import Mesh
from jax.sharding import PartitionSpec as P

ITERS = 3
NRHS = 4
BLOCKS = 16
STRIDE = NRHS + 1
LEAD = 8
ROWS = ("rows_0", "rows_1", "rows_2", "rows_3")
EPSILON = 1e-06

TOTALS = 4
TURNED = 3
COVER = 20_000_000_000
MIB = 1 << 20

WW = 3
GRAM = 4
NORM = 16

VMEM = pl.BlockSpec(memory_space=pltpu.VMEM)
SMEM = pl.BlockSpec(memory_space=pltpu.SMEM)
HBM = pl.BlockSpec(memory_space=pltpu.HBM)


def row_of(shape=(8, 128)):
    return lax.broadcasted_iota(jnp.int32, shape, 0)


def lane_of(shape=(8, 128)):
    return lax.broadcasted_iota(jnp.int32, shape, 1)


def split2(x):
    high = x.astype(jnp.bfloat16)
    return high, (x - high.astype(jnp.float32)).astype(jnp.bfloat16)


def split3(x):
    first = x.astype(jnp.bfloat16)
    second, third = split2(x - first.astype(jnp.float32))
    return first, second, third


def block(ref, r):
    return ref[pl.ds(8 * r, 8), :]


def in_group(group):
    row, lane = row_of(), lane_of()
    return (lane // NRHS == group) & (lane % NRHS == row % NRHS)


def row_of_sums(terms):
    row = jnp.zeros((8, 128), jnp.float32)
    for group, term in terms.items():
        row = row + jnp.where(in_group(group), jnp.sum(term, axis=1, keepdims=True), 0.0)
    return jnp.sum(jnp.where(row_of() < NRHS, row, 0.0), axis=0, keepdims=True)


def write_outgoing(outgoing, chosen, vector, sums=None):
    devices = chosen.shape[0]
    stride = outgoing.shape[0] // devices
    systems = [vector[pl.ds(k, BLOCKS, stride=8), :] for k in range(NRHS)]
    parts = jnp.concatenate(split3(jnp.concatenate(systems, axis=1)), axis=0)
    pick = jnp.concatenate([chosen[...][:, :BLOCKS]] * 3, axis=1)
    picked = jnp.dot(pick, parts, preferred_element_type=jnp.float32)
    for k in range(NRHS):
        rows = pl.ds(k, devices, stride=stride)
        outgoing[rows, :] = picked[:, k * 128 : (k + 1) * 128]
    if sums is not None:
        rows = pl.ds(NRHS, devices, stride=stride)
        outgoing[rows, :] = jnp.broadcast_to(sums, (devices, 128))


def begin_kernel(*refs):
    count, *given = refs[:5]
    wanted, own, *kept = refs[5:10]
    requests, right_side, copied = refs[10:]
    kept[-1][0] = count[0]
    copies = [
        pltpu.make_async_copy(source, target, copied.at[place])
        for place, (source, target) in enumerate(zip(given, [requests, right_side, *kept[:2]]))
    ]
    for copy in copies:
        copy.start()
    copies[0].wait()
    copies[1].wait()
    low_half = row_of() < NRHS
    squares = jnp.zeros((8, 128), jnp.float32)
    for j in range(BLOCKS // 2):
        both = block(right_side, j)
        turned = pltpu.roll(both, NRHS, 0)
        own[pl.ds(16 * j, 8), :] = jnp.where(low_half, both, turned)
        own[pl.ds(16 * j + 8, 8), :] = jnp.where(low_half, turned, both)
        squares = squares + both * both
    sums = row_of_sums({NORM: squares + pltpu.roll(squares, NRHS, 0)})
    ids = jnp.broadcast_to(requests[...], wanted.shape).T.astype(jnp.float32)
    is_norm = lane_of(wanted.shape) // NRHS == NORM
    wanted[...] = jnp.where(is_norm, jnp.broadcast_to(sums, wanted.shape), ids)
    for copy in copies[2:]:
        copy.wait()


def first_kernel(own, asked, chosen, sums, outgoing):
    hot = asked[...] == lane_of(asked.shape).astype(jnp.float32)
    chosen[...] = hot.astype(jnp.float32).astype(jnp.bfloat16)
    sums[...] = jnp.broadcast_to(jnp.sum(asked[...], axis=0, keepdims=True), sums.shape)
    write_outgoing(outgoing, chosen, own)


def coefficients(rows):
    def entry(row, group):
        chosen = jnp.where(in_group(group), row, 0.0)
        return jnp.broadcast_to(jnp.sum(chosen, axis=1, keepdims=True), (8, 128))

    beta = jnp.sqrt(entry(rows[0], NORM) + EPSILON)
    columns = []
    gram = {}
    for column, row in enumerate(rows[1:]):
        dots = [entry(row, i) for i in range(column + 1)]
        for i in range(column + 1):
            gram[i, column] = gram[column, i] = entry(row, GRAM + i)
        h = []
        for i in range(column + 1):
            value = dots[i]
            for l in range(i):
                value = value - h[l] * gram[l, i]
            h.append(value)
        left = entry(row, WW)
        for i in range(column + 1):
            left = left - h[i] * dots[i]
        for i in range(column + 1):
            residue = dots[i]
            for l in range(column + 1):
                residue = residue - h[l] * gram[l, i]
            left = left - h[i] * residue
        columns.append((h, jnp.sqrt(jnp.maximum(left, 0.0) + EPSILON)))
    return beta, columns


def strided(values):
    of_system = [jnp.broadcast_to(values[k : k + 1], (8, 128)) for k in range(NRHS)]
    groups = []
    for group in range(STRIDE):
        system = (row_of() + 8 * group) % STRIDE
        chosen = of_system[NRHS - 1]
        for k in range(NRHS - 1):
            chosen = jnp.where(system == k, of_system[k], chosen)
        groups.append(chosen)
    return jnp.concatenate(groups, axis=0)


def step_kernel(step, last, *refs):
    refs = list(refs)

    def take(size):
        taken = refs[:size]
        del refs[:size]
        return taken

    count, tiles = take(2) if step == 0 else (None, None)
    packed = refs.pop(0) if step > 0 else None
    slots, rows_of, chosen, incoming, own = take(5)
    earlier_sums, earlier_own, earlier_halo = take(max(step, 1)), take(step), take(step)
    basis_own, outgoing = take(2)
    if step > 0:
        (sums_out,) = take(1)
    if not last:
        basis_halo, product = take(2)
    if step == 0:
        packed = refs.pop(0)
    (table,) = take(1)
    totals = take(TOTALS)
    if last:
        basis_halo, product = take(2)
    devices = table.shape[0] // 8 - BLOCKS

    def pack(tile_id, target, start):
        tile = jnp.where(tile_id < live, tiles[tile_id], 0.0)
        high, low = split2(tile.T)
        both = jnp.concatenate([high, low], axis=0)
        target[pl.ds(start, 256), :] = both
        return both

    def turn(left, tile_id, target, start):
        sides = [jnp.where(tile_id + side < live, tiles[tile_id + side], 0.0) for side in range(2)]
        right = jnp.concatenate([jnp.concatenate(split2(tile), axis=1) for tile in sides], axis=0)
        result = lax.dot_general(
            jnp.concatenate([left, identity[...]], axis=0),
            right,
            (((1,), (1,)), ((), ())),
            preferred_element_type=jnp.float32,
        )
        turned = result[16:].astype(jnp.bfloat16)
        target[pl.ds(start, 256), :] = turned[:, :128]
        target[pl.ds(start + 256, 256), :] = turned[:, 128:]
        return result[:16]

    def multiply(tile):
        own_slots = BLOCKS + devices
        picked = [
            table[pl.ds(8 * tile if tile < own_slots else pl.multiple_of(slots[tile] * 8, 8), 8), :]
            for tile in (tile, tile + 1)
        ]
        left = jnp.concatenate(picked, axis=0).astype(jnp.bfloat16)
        left = jnp.concatenate([left, left], axis=1)
        start = tile * 256
        if step == 0 and tile // 2 % TURNED == 0:
            result = turn(left, tile, packed, start)
        else:
            if step == 0:
                right = [pack(tile + side, packed, start + side * 256) for side in range(2)]
            else:
                right = [packed[pl.ds(start + side * 256, 256), :] for side in range(2)]
            result = jnp.dot(
                left, jnp.concatenate(right, axis=1), preferred_element_type=jnp.float32
            )
        for side in range(2):
            total = totals[(tile + side) % TOTALS]
            row = tile + side
            row = 8 * row if row < BLOCKS else pl.multiple_of(rows_of[row] * 8, 8)
            part = result[side * 8 : side * 8 + 8, side * 128 : side * 128 + 128]
            total[pl.ds(row, 8), :] += part

    if step == 0:
        live = count[0]
        (identity,) = take(1)
        diagonal = row_of((256, 256)) == lane_of((256, 256))
        identity[...] = diagonal.astype(jnp.float32).astype(jnp.bfloat16)

    sums_rows = [ref[...] for ref in earlier_sums]
    if step > 0:
        rows = pl.ds(NRHS, devices, stride=STRIDE)
        sums_rows.append(jnp.sum(incoming[rows, :], axis=0, keepdims=True))
        sums_out[...] = jnp.broadcast_to(sums_rows[-1], (8, 128))
    beta, columns = coefficients(sums_rows)
    h, length = columns[-1] if step else ([], beta)
    scale = 1.0 / length
    for total in totals:
        total[...] = jnp.zeros_like(total)
    low_half = row_of() < NRHS

    def entry(value):
        high = value.astype(jnp.bfloat16).astype(jnp.float32)
        return jnp.where(low_half, high, value - high)

    for r in range(BLOCKS):
        value = block(own, r)
        for i in range(step):
            value = value - h[i] * block(earlier_own[i], r)
        value = value * scale
        basis_own[pl.ds(8 * r, 8), :] = value
        table[pl.ds(8 * r, 8), :] = entry(value)
    if step == 0:
        for j in range(devices // 2):
            both = block(incoming, j) * scale
            turned = pltpu.roll(both, NRHS, 0)
            for side in range(2):
                value = jnp.where(low_half, turned, both) if side else jnp.where(low_half, both, turned)
                device = 2 * j + side
                basis_halo[pl.ds(LEAD + STRIDE * device, 8), :] = value
                table[pl.ds(8 * (BLOCKS + device), 8), :] = entry(value)
    else:
        wide_scale = strided(scale)
        wide_h = [strided(value) for value in h]
        period = 8 * STRIDE
        for group in range(devices // 8):
            value = incoming[pl.ds(period * group, period), :]
            rows = pl.ds(LEAD + period * group, period)
            for i in range(step):
                value = value - wide_h[i] * earlier_halo[i][rows, :]
            basis_halo[rows, :] = value * wide_scale
        for device in range(devices):
            start = LEAD + STRIDE * device
            upper = basis_halo[pl.ds(start, 8), :]
            lower = basis_halo[pl.ds(start - NRHS, 8), :]
            table[pl.ds(8 * (BLOCKS + device), 8), :] = entry(jnp.where(low_half, upper, lower))

    for tile in range(0, packed.shape[0] // 256, 2):
        multiply(tile)

    blocks = []
    for r in range(BLOCKS):
        value = functools.reduce(jnp.add, [block(total, r) for total in totals])
        value = value + pltpu.roll(value, NRHS, 0)
        product[pl.ds(8 * r, 8), :] = value
        blocks.append(value)
    terms = {WW: functools.reduce(jnp.add, [b * b for b in blocks])}
    for i, vector in enumerate([*earlier_own, basis_own]):
        known = [block(vector, r) for r in range(BLOCKS)]
        latest = [block(basis_own, r) for r in range(BLOCKS)]
        terms[i] = functools.reduce(jnp.add, [a * b for a, b in zip(known, blocks)])
        terms[GRAM + i] = functools.reduce(jnp.add, [a * b for a, b in zip(known, latest)])
    local = row_of_sums(terms)
    if last:
        outgoing[...] = jnp.broadcast_to(local, outgoing.shape)
    else:
        write_outgoing(outgoing, chosen, product, local)


def weights_of(beta, columns):
    rotations = []
    triangle = []
    target = [beta]
    for column, (h, length) in enumerate(columns):
        values = list(h) + [length]
        for earlier, (cosine, sine) in enumerate(rotations):
            first, second = values[earlier], values[earlier + 1]
            values[earlier] = cosine * first + sine * second
            values[earlier + 1] = cosine * second - sine * first
        first, second = values[column], values[column + 1]
        radius = jnp.sqrt(first * first + second * second)
        cosine, sine = first / radius, second / radius
        rotations.append((cosine, sine))
        triangle.append(values[:column] + [radius])
        leading = target[column]
        target[column] = cosine * leading
        target.append(-sine * leading)
    size = len(columns)
    weights = [None] * size
    for column in reversed(range(size)):
        value = target[column]
        for later in range(column + 1, size):
            value = value - triangle[later][column] * weights[later]
        weights[column] = value / triangle[column][column]
    return weights


def final_kernel(incoming, *refs):
    earlier_sums, bases = refs[:ITERS], refs[ITERS : 2 * ITERS]
    solution, hessenberg = refs[2 * ITERS :]
    sums = jnp.sum(incoming[...], axis=0, keepdims=True)
    beta, columns = coefficients([ref[...] for ref in earlier_sums] + [sums])
    weights = weights_of(beta, columns)

    def combined(r):
        value = weights[0] * block(bases[0], r)
        for weight, basis in zip(weights[1:], bases[1:]):
            value = value + weight * block(basis, r)
        return value

    for j in range(BLOCKS // 2):
        both = jnp.where(row_of() < NRHS, combined(2 * j), combined(2 * j + 1))
        solution[pl.ds(8 * j, 8), :] = both
    for column, (h, length) in enumerate(columns):
        table = jnp.zeros((8, 128), jnp.float32)
        for i, value in enumerate([*h, length]):
            table = jnp.where(lane_of() == i, value, table)
        hessenberg[column] = table[:NRHS, : ITERS + 1]


def params(limit):
    return pltpu.CompilerParams(vmem_limit_bytes=limit * MIB)


def in_hbm(array):
    return pltpu.with_memory_space_constraint(array, pltpu.HBM)


def exchange(outgoing):
    size = outgoing.shape[0]
    moved = lax.all_to_all(
        outgoing.reshape(size, 1, 128), ROWS, split_axis=0, concat_axis=0, tiled=True
    )
    return moved.reshape(size, 128)


def on_device(tile_values, tile_row, tile_slot, tile_count, requests, right_side):
    devices = lax.axis_size(ROWS)
    tiles = tile_values.shape[0]
    f32 = jnp.float32
    flat = right_side.reshape(BLOCKS * NRHS, 128)
    block_rows = jax.ShapeDtypeStruct((8 * BLOCKS, 128), f32)
    sum_rows = jax.ShapeDtypeStruct((8, 128), f32)
    message = jax.ShapeDtypeStruct((devices * STRIDE, 128), f32)
    halo_rows = jax.ShapeDtypeStruct((LEAD + devices * STRIDE + 8, 128), f32)
    wanted, own, *kept = pl.pallas_call(
        begin_kernel,
        out_shape=(
            jax.ShapeDtypeStruct((devices, 128), f32),
            block_rows,
            pltpu.SMEM(tile_slot.shape, tile_slot.dtype),
            pltpu.SMEM(tile_row.shape, tile_row.dtype),
            pltpu.SMEM(tile_count.shape, tile_count.dtype),
        ),
        in_specs=[SMEM] + [HBM] * 4,
        out_specs=(VMEM, VMEM, SMEM, SMEM, SMEM),
        scratch_shapes=[
            pltpu.VMEM((1, devices), jnp.int32),
            pltpu.VMEM(flat.shape, f32),
            pltpu.SemaphoreType.DMA((4,)),
        ],
        compiler_params=params(8),
        name="begin",
    )(tile_count, *map(in_hbm, (requests.reshape(1, devices), flat, tile_slot, tile_row)))
    slots, rows_of, count = kept
    asked = exchange(wanted)
    chosen, norms, outgoing = pl.pallas_call(
        first_kernel,
        out_shape=(
            jax.ShapeDtypeStruct((devices, devices), jnp.bfloat16),
            sum_rows,
            jax.ShapeDtypeStruct((devices * NRHS, 128), f32),
        ),
        in_specs=[VMEM, VMEM],
        out_specs=(VMEM, VMEM, VMEM),
        compiler_params=params(8),
        cost_estimate=pl.CostEstimate(flops=COVER, bytes_accessed=0, transcendentals=0),
        name="first",
    )(own, asked)
    sums, owns, halos = [norms], [], []
    packed = None
    for step in range(ITERS):
        last = step == ITERS - 1
        incoming = exchange(outgoing)
        shapes = [block_rows]
        shapes += [jax.ShapeDtypeStruct((devices, 128), f32)] if last else [message]
        shapes += [sum_rows] if step > 0 else []
        shapes += [] if last else [halo_rows, block_rows]
        scratch = [pltpu.VMEM((8 * (BLOCKS + devices), 128), f32)]
        scratch += [pltpu.VMEM(block_rows.shape, f32)] * TOTALS
        if last:
            scratch += [pltpu.VMEM(halo_rows.shape, f32), pltpu.VMEM(block_rows.shape, f32)]
        operands = [slots, rows_of, chosen, incoming, own, *sums, *owns, *halos]
        specs = [SMEM, SMEM] + [VMEM] * (len(operands) - 2)
        if step == 0:
            scratch.append(pltpu.VMEM((256, 256), jnp.bfloat16))
            shapes.append(pltpu.VMEM((tiles * 256, 128), jnp.bfloat16))
            operands = [count, tile_values] + operands
            specs = [SMEM, VMEM] + specs
        else:
            operands = [packed] + operands
            specs = [VMEM] + specs
        vector, outgoing, *kept = pl.pallas_call(
            functools.partial(step_kernel, step, last),
            out_shape=shapes,
            in_specs=specs,
            out_specs=[VMEM] * len(shapes),
            scratch_shapes=scratch,
            compiler_params=params(20),
            name=f"step{step}",
        )(*operands)
        if step > 0:
            sums.append(kept.pop(0))
        owns.append(vector)
        if not last:
            halo, own, *rest = kept
            halos.append(halo)
            packed = rest[0] if step == 0 else packed
    incoming = exchange(outgoing)
    solution, hessenberg = pl.pallas_call(
        final_kernel,
        out_shape=(
            jax.ShapeDtypeStruct(flat.shape, f32),
            jax.ShapeDtypeStruct((ITERS, NRHS, ITERS + 1), f32),
        ),
        in_specs=[VMEM] * (1 + 2 * ITERS),
        out_specs=(VMEM, VMEM),
        compiler_params=params(8),
        name="final",
    )(incoming, *sums, *owns)
    return solution.reshape(right_side.shape), hessenberg.transpose(1, 2, 0)


def solution(mesh):
    finer = Mesh(mesh.devices.reshape(4, 4, 4, 2), ROWS)
    placed = (
        P(ROWS, None, None),
        P(ROWS),
        P(ROWS),
        P(ROWS),
        P(ROWS, None, None),
        P(ROWS, None, None),
    )
    return jax.shard_map(
        on_device,
        mesh=finer,
        in_specs=placed,
        out_specs=(P(ROWS, None, None), P()),
        check_vma=False,
    )
```
